256 devices in a mesh: blk: 64 (over x, z, y_hi), dp: 4 (over y_lo, core).
Axes of the slice: x: 4, y: 4 (y_hi: 2, y_lo: 2; y = y_hi * 2 + y_lo), z: 8, core: 2. Of those that a mesh axis runs over, the one named last changes fastest.
Arguments:
- images: bfloat16 [32768, 768], P(('dp', 'blk')), parts along dimension 0, may hold values from -4 to 4
- texts: bfloat16 [32768, 768], P(('dp', 'blk')), parts along dimension 0, may hold values from -4 to 4
- scale: float32 [1], replicated, may hold values from 10 to 20
- cotangent: float32 [2, 32768], P(None, ('dp', 'blk')), parts along dimension 1, may hold values from 0.5 to 2
Outputs:
- row_losses: float32 [2, 32768], P(None, ('dp', 'blk')), parts along dimension 1
- grad_images: float32 [32768, 768], P(('dp', 'blk')), parts along dimension 0
- grad_texts: float32 [32768, 768], P(('dp', 'blk')), parts along dimension 0
The draws below stay inside these ranges and needn't reach their ends.
There are 4 independent parts, one for each index of `dp`. The reference program is written for one: setup_inputs(seed, part) draws one part's arguments, and reference() takes and returns one part's arrays. A program takes and returns all parts, laid end to end along the dimension named above; an argument that names none is the same for every part. Nothing has to cross between parts.
All inputs are finite; a program needn't handle non-finite values.
Results may differ from the reference program's by a relative error of at most 0.0019.
Values may be sent and summed in bfloat16 or wider, within the bound.
No kernel may reach another device: no remote copies, remote signals or barrier semaphores. Data moves between devices by JAX's collectives and lax.ppermute only.
A program may use at most 64 MiB of HBM per device.

```python
import math
import jax
import jax.numpy as jnp
from jax import lax

WIDTH = 768
BATCH = 8192


def embed_pair(key):
    base_key = jax.random.fold_in(key, 11)
    keys = jax.random.split(base_key, 2)
    images = jnp.clip(0.05 * jax.random.normal(keys[0], (BATCH, WIDTH), jnp.float32), -0.3, 0.3)
    texts = jnp.clip(0.05 * jax.random.normal(keys[1], (BATCH, WIDTH), jnp.float32), -0.3, 0.3)
    return (jnp.clip(images, -4.0, 4.0), jnp.clip(texts, -4.0, 4.0))


def draw_images(key, part):
    return embed_pair(key)[0].astype(jnp.bfloat16)


def draw_texts(key, part):
    return embed_pair(key)[1].astype(jnp.bfloat16)


def shard_levels(rng, dims, pieces, least, largest):
    factor_of = 1.0
    for axis_at, parts in pieces:
        draws = jax.random.uniform(jax.random.fold_in(jax.random.fold_in(rng, 6), axis_at), (parts,), jnp.float32, least / len(pieces), largest / len(pieces))
        factor_of = factor_of * jnp.repeat(jnp.exp(draws), dims[axis_at] // parts).reshape((-1,) + (1,) * (len(dims) - 1 - axis_at))
    return factor_of


def setup_inputs(seed: int = 0, part: int = 0) -> dict:
    key_of = jax.random.split(jax.random.key(seed), 5)
    own_keys = jax.random.split(jax.random.fold_in(key_of[4], part), 5)
    images = draw_images(jax.random.fold_in(jax.random.fold_in(key_of[4], part), 71), part)
    texts = draw_texts(jax.random.fold_in(jax.random.fold_in(key_of[4], part), 71), part)
    scale = jnp.clip(jax.random.uniform(key_of[2], (1,), jnp.float32, 10.0, 20.0), 10.0, 20.0)
    cotangent = jnp.clip(jnp.exp(math.log(2.0) - 1.3862944 * jax.random.uniform(own_keys[3], (2, BATCH), jnp.float32) ** shard_levels(own_keys[3], (2, BATCH), ((1, 64),), -0.2, 0.2)), 0.5, 2.0)
    return {"images": images, "texts": texts, "scale": scale, "cotangent": cotangent}


def lse_blocks(left, right, logit_scale, span):
    def one_block(block):
        scores = logit_scale * jnp.dot(block, right.T, preferred_element_type=jnp.float32)
        top_value = jnp.max(scores, axis=1, keepdims=True)
        return (top_value + jnp.log(jnp.sum(jnp.exp(scores - top_value), axis=1, keepdims=True)))[:, 0]
    blocked = left.reshape(left.shape[0] // span, span, left.shape[1])
    return lax.map(one_block, blocked).reshape(left.shape[0])


def grad_blocks(left, right, own_lse, own_cot, other_lse, other_cot, logit_scale, span):
    def one_block(packed):
        block, lse_block, cot_block = packed
        scores = logit_scale * jnp.dot(block, right.T, preferred_element_type=jnp.float32)
        weights = cot_block[:, None] * jnp.exp(scores - lse_block[:, None]) + other_cot[None, :] * jnp.exp(scores - other_lse[None, :])
        return jnp.dot(weights.astype(jnp.bfloat16), right, preferred_element_type=jnp.float32)
    count = left.shape[0] // span
    packed = (left.reshape(count, span, left.shape[1]), own_lse.reshape(count, span), own_cot.reshape(count, span))
    return lax.map(one_block, packed).reshape(left.shape[0], right.shape[1])


def reference(images, texts, scale, cotangent):
    logit_scale = scale[0]
    span = math.gcd(images.shape[0], 512)
    row_lse = lse_blocks(images, texts, logit_scale, span)
    col_lse = lse_blocks(texts, images, logit_scale, span)
    matched = logit_scale * jnp.sum(images.astype(jnp.float32) * texts.astype(jnp.float32), axis=1)
    row_losses = jnp.stack([row_lse - matched, col_lse - matched])
    cot_rows = cotangent[0]
    cot_cols = cotangent[1]
    both_cot = (cot_rows + cot_cols)[:, None]
    image_terms = grad_blocks(images, texts, row_lse, cot_rows, col_lse, cot_cols, logit_scale, span)
    text_terms = grad_blocks(texts, images, col_lse, cot_cols, row_lse, cot_rows, logit_scale, span)
    grad_images = logit_scale * (image_terms - both_cot * texts.astype(jnp.float32))
    grad_texts = logit_scale * (text_terms - both_cot * images.astype(jnp.float32))
    return row_losses, grad_images, grad_texts
```

```python
import jax
import jax.numpy as jnp
from jax import lax
from jax.sharding import Mesh, PartitionSpec as P

ROWS = "z"
COLS = ("x", "h")


def spread(value, axis):
    copies = jnp.broadcast_to(value[None], (lax.axis_size(axis),) + value.shape)
    return lax.all_to_all(copies, axis, 0, 0, tiled=True)


def merge_lse(parts):
    top = jnp.max(parts, axis=0)
    return top + jnp.log(jnp.sum(jnp.exp(parts - top[None]), axis=0))


def shards(images, texts, scale, cotangent):
    n = images.shape[0]
    width = images.shape[1]
    logit_scale = scale[0]
    row_n = lax.axis_size(ROWS)
    col_n = lax.axis_size(COLS)
    img = spread(images, ROWS).reshape(row_n * n, width)
    txt = spread(texts, COLS).reshape(col_n * n, width)
    scores = logit_scale * lax.dot_general(
        img, txt, (((1,), (1,)), ((), ())), preferred_element_type=jnp.float32
    )
    row_top = jnp.max(scores, axis=1)
    row_part = row_top + jnp.log(jnp.sum(jnp.exp(scores - row_top[:, None]), axis=1))
    col_top = jnp.max(scores, axis=0)
    col_part = col_top + jnp.log(jnp.sum(jnp.exp(scores - col_top[None, :]), axis=0))
    row_msg = jnp.concatenate([row_part.reshape(row_n, n), cotangent[:1]], axis=0)
    col_msg = jnp.concatenate([col_part.reshape(col_n, n), cotangent[1:]], axis=0)
    row_all = spread(row_msg, ROWS)
    col_all = spread(col_msg, COLS)
    row_lse = merge_lse(row_all[:, :row_n])
    col_lse = merge_lse(col_all[:, :col_n])
    row_cot = row_all[:, row_n].reshape(-1)
    col_cot = col_all[:, col_n].reshape(-1)
    weights = row_cot[:, None] * jnp.exp(scores - row_lse.reshape(-1)[:, None]) + col_cot[
        None, :
    ] * jnp.exp(scores - col_lse.reshape(-1)[None, :])
    weights = weights.astype(jnp.bfloat16)
    img_part = jnp.dot(weights, txt, preferred_element_type=jnp.float32).astype(jnp.bfloat16)
    txt_part = lax.dot_general(
        weights, img, (((0,), (0,)), ((), ())), preferred_element_type=jnp.float32
    ).astype(jnp.bfloat16)
    img_sent = lax.all_to_all(img_part.reshape(row_n, n, width), ROWS, 0, 0, tiled=True)
    txt_sent = lax.all_to_all(txt_part.reshape(col_n, n, width), COLS, 0, 0, tiled=True)
    wide_i = images.astype(jnp.float32)
    wide_t = texts.astype(jnp.float32)
    matched = logit_scale * jnp.sum(wide_i * wide_t, axis=1)
    own_row = lax.dynamic_index_in_dim(row_lse, lax.axis_index(ROWS), 0, keepdims=False)
    own_col = lax.dynamic_index_in_dim(col_lse, lax.axis_index(COLS), 0, keepdims=False)
    row_losses = jnp.stack([own_row - matched, own_col - matched])
    both_cot = (cotangent[0] + cotangent[1])[:, None]
    grad_images = logit_scale * (
        jnp.sum(img_sent.astype(jnp.float32), axis=0) - both_cot * wide_t
    )
    grad_texts = logit_scale * (
        jnp.sum(txt_sent.astype(jnp.float32), axis=0) - both_cot * wide_i
    )
    return (row_losses, grad_images, grad_texts)


def solution(mesh):
    grid = Mesh(mesh.devices.reshape(4, 8, 2, 4), ("x", "z", "h", "dp"))
    rows = ("dp", "x", "z", "h")
    return jax.shard_map(
        shards,
        mesh=grid,
        in_specs=(P(rows, None), P(rows, None), P(), P(None, rows)),
        out_specs=(P(None, rows), P(rows, None), P(rows, None)),
        check_vma=False,
    )
```

```python
import jax
import jax.numpy as jnp
from jax import lax
from jax.sharding import Mesh, PartitionSpec as P


def moved(value, axis, steps):
    count = lax.axis_size(axis)
    return lax.ppermute(value, axis, [(i, (i + steps) % count) for i in range(count)])


def swapped(value, axis, bit):
    count = lax.axis_size(axis)
    return lax.ppermute(value, axis, [(i, i ^ bit) for i in range(count)])


def gather_z(block):
    half = lax.axis_size("z") // 2
    held = {0: block}
    for k in range(1, half):
        held[-k] = moved(held[1 - k], "z", 1)
        held[k] = moved(held[k - 1], "z", -1)
    held[half] = moved(held[half - 1], "z", -1)
    return held


def gather_xh(block):
    pair = jnp.concatenate([block, moved(block, "h", 1)], axis=0)
    n = block.shape[0]
    fore = moved(pair, "x", -1)
    back = moved(pair, "x", 1)
    far = jnp.concatenate([moved(fore[:n], "x", -1), moved(back[n:], "x", 1)], axis=0)
    return {0: pair, 1: fore, 2: far, 3: back}


def low(value):
    return value.astype(jnp.bfloat16)


def wide(value):
    return value.astype(jnp.float32)


def reduce_z(parts):
    half = lax.axis_size("z") // 2
    up = moved(low(parts[half]), "z", 1)
    down = None
    for k in range(half - 1, 0, -1):
        up = moved(low(parts[k] + wide(up)), "z", 1)
        down = moved(low(parts[-k] if down is None else parts[-k] + wide(down)), "z", -1)
    return parts[0] + wide(up) + wide(down)


def reduce_xh(parts, n):
    up = moved(low(parts[2][:n]), "x", 1)
    down = moved(low(parts[2][n:]), "x", -1)
    fore = jnp.concatenate([parts[1][:n] + wide(up), parts[1][n:]], axis=0)
    back = jnp.concatenate([parts[3][:n], parts[3][n:] + wide(down)], axis=0)
    fore = moved(low(fore), "x", 1)
    back = moved(low(back), "x", -1)
    total = parts[0] + wide(fore) + wide(back)
    return total[:n] + wide(moved(low(total[n:]), "h", 1))


def merge_lse(first, second):
    top = jnp.maximum(first, second)
    return top + jnp.log(jnp.exp(first - top) + jnp.exp(second - top))


def shards(images, texts, scale, cotangent):
    n, width = images.shape
    logit_scale = scale[0]
    at_z, at_x, at_h = (lax.axis_index(a) for a in ("z", "x", "h"))
    z_n, x_n = lax.axis_size("z"), lax.axis_size("x")
    half = z_n // 2
    offs = [0] + [s * k for k in range(1, half) for s in (1, -1)] + [half]
    img_held = gather_z(images)
    txt_held = gather_xh(texts)
    img = jnp.concatenate([img_held[o] for o in offs], axis=0)
    txt = jnp.concatenate([txt_held[d] for d in (0, 1, 3, 2)], axis=0)
    z_ids = jnp.stack([(at_z + o) % z_n for o in offs])
    c_ids = jnp.stack([((at_x + d) % x_n) * 2 + (at_h ^ e) for d in (0, 1, 3, 2) for e in (0, 1)])
    z_hot = (z_ids[:, None] == jnp.arange(z_n)[None, :])[:, :, None]
    c_hot = (c_ids[:, None] == jnp.arange(2 * x_n)[None, :])[:, :, None]
    scores = logit_scale * lax.dot_general(
        img, txt, (((1,), (1,)), ((), ())), preferred_element_type=jnp.float32
    )
    row_top = jnp.max(scores, axis=1)
    row_part = row_top + jnp.log(jnp.sum(jnp.exp(scores - row_top[:, None]), axis=1))
    col_top = jnp.max(scores, axis=0)
    col_part = col_top + jnp.log(jnp.sum(jnp.exp(scores - col_top[None, :]), axis=0))

    def placed(value, hot):
        return jnp.sum(jnp.where(hot, value.reshape(-1, n)[:, None, :], 0.0), axis=0)

    def taken(value, hot):
        return jnp.sum(jnp.where(hot, value[None, :, :], 0.0), axis=1).reshape(-1)

    row_abs = placed(row_part, z_hot)
    col_abs = placed(col_part, c_hot)
    row_cot = jnp.where(z_hot[0], cotangent[:1], 0.0)
    col_cot = jnp.where(c_hot[0], cotangent[1:], 0.0)
    row_msg = jnp.concatenate([row_abs, row_cot], axis=0)
    col_msg = jnp.concatenate([col_abs, col_cot], axis=0)
    for z_bit, col_axis, col_bit in ((1, "h", 1), (2, "x", 1), (4, "x", 2)):
        row_got = swapped(row_msg, "z", z_bit)
        col_got = swapped(col_msg, col_axis, col_bit)
        row_msg = jnp.concatenate(
            [merge_lse(row_msg[:z_n], row_got[:z_n]), row_msg[z_n:] + row_got[z_n:]], axis=0
        )
        c_n = 2 * x_n
        col_msg = jnp.concatenate(
            [merge_lse(col_msg[:c_n], col_got[:c_n]), col_msg[c_n:] + col_got[c_n:]], axis=0
        )
    row_lse, row_cot = taken(row_msg[:z_n], z_hot), taken(row_msg[z_n:], z_hot)
    col_lse, col_cot = taken(col_msg[: 2 * x_n], c_hot), taken(col_msg[2 * x_n :], c_hot)
    weights = row_cot[:, None] * jnp.exp(scores - row_lse[:, None]) + col_cot[None, :] * jnp.exp(
        scores - col_lse[None, :]
    )
    weights = low(weights)
    img_part = jnp.dot(weights, txt, preferred_element_type=jnp.float32)
    txt_part = lax.dot_general(
        weights, img, (((0,), (0,)), ((), ())), preferred_element_type=jnp.float32
    )
    img_terms = reduce_z({o: img_part[i * n : (i + 1) * n] for i, o in enumerate(offs)})
    txt_terms = reduce_xh(
        {d: txt_part[2 * i * n : 2 * (i + 1) * n] for i, d in enumerate((0, 1, 3, 2))}, n
    )
    matched = logit_scale * jnp.sum(wide(images) * wide(texts), axis=1)
    row_losses = jnp.stack([row_lse[:n] - matched, col_lse[:n] - matched])
    both_cot = (cotangent[0] + cotangent[1])[:, None]
    grad_images = logit_scale * (img_terms - both_cot * wide(texts))
    grad_texts = logit_scale * (txt_terms - both_cot * wide(images))
    return (row_losses, grad_images, grad_texts)


def solution(mesh):
    grid = Mesh(mesh.devices.reshape(4, 8, 2, 4), ("x", "z", "h", "dp"))
    rows = ("dp", "x", "z", "h")
    return jax.shard_map(
        shards,
        mesh=grid,
        in_specs=(P(rows, None), P(rows, None), P(), P(None, rows)),
        out_specs=(P(None, rows), P(rows, None), P(rows, None)),
        check_vma=False,
    )
```

```python
import functools

import jax
import jax.numpy as jnp
from jax import lax
from jax.experimental import pallas as pl
from jax.experimental.pallas import tpu as pltpu
from jax.sharding import Mesh, PartitionSpec as P

VMEM = pl.BlockSpec(memory_space=pltpu.VMEM)
SMEM = pl.BlockSpec(memory_space=pltpu.SMEM)
PARAMS = pltpu.CompilerParams(vmem_limit_bytes=24 * 1024 * 1024)


def moved(value, axis, steps):
    count = lax.axis_size(axis)
    return lax.ppermute(value, axis, [(i, (i + steps) % count) for i in range(count)])


def swapped(value, axis, bit):
    count = lax.axis_size(axis)
    return lax.ppermute(value, axis, [(i, i ^ bit) for i in range(count)])


def gather_z(block):
    half = lax.axis_size("z") // 2
    held = {0: block}
    for k in range(1, half):
        held[-k] = moved(held[1 - k], "z", 1)
        held[k] = moved(held[k - 1], "z", -1)
    held[half] = moved(held[half - 1], "z", -1)
    return held


def gather_xh(block):
    held = {(0, 0): block, (0, 1): moved(block, "h", 1)}
    for e in (0, 1):
        held[1, e] = moved(held[0, e], "x", -1)
        held[3, e] = moved(held[0, e], "x", 1)
    held[2, 0] = moved(held[1, 0], "x", -1)
    held[2, 1] = moved(held[3, 1], "x", 1)
    return held


def low(value):
    return value.astype(jnp.bfloat16)


def wide(value):
    return value.astype(jnp.float32)


def across(column):
    return jnp.broadcast_to(column, (column.shape[0], 128)).T[0:1, :]


def down(row):
    return jnp.broadcast_to(row, (128, row.shape[1])).T


def product(left, right, left_dim, right_dim):
    return lax.dot_general(
        left, right, (((left_dim,), (right_dim,)), ((), ())), preferred_element_type=jnp.float32
    )


def row_stats(s, row_ref, at, col_top):
    top = jnp.max(s, axis=1, keepdims=True)
    total = jnp.sum(jnp.exp(s - top), axis=1, keepdims=True)
    row_ref[at : at + 1, :] = across(top + jnp.log(total))
    return jnp.sum(jnp.exp(s - col_top), axis=0, keepdims=True)


def stats_a_kernel(blocks, *refs):
    scale_ref = refs[0]
    img_refs, refs = refs[1 : 1 + blocks], refs[1 + blocks :]
    txt_refs = refs[:-6]
    s_ref, row_ref, top_ref, sum_ref, img_ref, txt_ref = refs[-6:]
    logit_scale = scale_ref[0]
    for b, ref in enumerate(img_refs):
        img_ref[128 * b : 128 * b + 128, :] = ref[...]
    for c, ref in enumerate(txt_refs):
        txt_ref[128 * c : 128 * c + 128, :] = ref[...]
    for c in range(0, txt_ref.shape[0], 256):
        part = product(img_ref[...], txt_ref[c : c + 256, :], 1, 1)
        s_ref[:, c : c + 256] = logit_scale * part
    col_top = jnp.max(s_ref[...], axis=0, keepdims=True)
    col_sum = jnp.zeros_like(col_top)
    for b in range(blocks):
        col_sum = col_sum + row_stats(s_ref[128 * b : 128 * b + 128, :], row_ref, b, col_top)
    top_ref[...] = col_top
    sum_ref[...] = col_sum


def stats_b_kernel(scale_ref, img_ref, txt_ref, top_ref, sum_ref, s_ref, row_ref, col_ref):
    s = scale_ref[0] * product(img_ref[...], txt_ref[...], 1, 1)
    s_ref[...] = s
    col_top = jnp.maximum(jnp.max(s, axis=0, keepdims=True), top_ref[...])
    col_sum = row_stats(s, row_ref, 0, col_top) + sum_ref[...] * jnp.exp(top_ref[...] - col_top)
    lse = col_top + jnp.log(col_sum)
    for c in range(0, lse.shape[1], 128):
        col_ref[c // 128 : c // 128 + 1, :] = lse[:, c : c + 128]


def weights_kernel(
    sa_ref, sb_ref, row_ref, col_ref, img_a, img_b, txt_ref, wa_ref, wb_ref, *first_refs
):
    blocks = row_ref.shape[0] // 2
    cols = col_ref.shape[0] // 2
    for b in range(blocks - 1, -1, -1):
        row_lse = down(row_ref[b : b + 1, :])
        row_cot = down(row_ref[blocks + b : blocks + b + 1, :])
        last = b == blocks - 1
        s_ref, w_ref, r = (sb_ref, wb_ref, 0) if last else (sa_ref, wa_ref, 128 * b)
        for c in range(cols):
            s = s_ref[r : r + 128, 128 * c : 128 * c + 128]
            w = row_cot * jnp.exp(s - row_lse) + col_ref[cols + c : cols + c + 1, :] * jnp.exp(
                s - col_ref[c : c + 1, :]
            )
            w_ref[r : r + 128, 128 * c : 128 * c + 128] = low(w)
    width = wa_ref.shape[1]
    firsts = jnp.concatenate([wa_ref[wa_ref.shape[0] - 128 :, :], wb_ref[...]], axis=0)
    image_part = product(firsts, txt_ref[...], 1, 0)
    text_part = product(wa_ref[:, width - 256 :], img_a[...], 0, 0) + product(
        wb_ref[:, width - 256 :], img_b[...], 0, 0
    )
    for k, ref in enumerate(first_refs):
        part = (image_part, text_part)[k // 2]
        ref[...] = low(part[128 * (k % 2) : 128 * (k % 2) + 128, :])


def rest_kernel(rows, cols, wa_ref, wb_ref, img_a, img_b, txt_ref, *out_refs):
    image_part = product(wa_ref[: 128 * rows, :], txt_ref[...], 1, 0)
    text_part = product(wa_ref[:, : 128 * cols], img_a[...], 0, 0) + product(
        wb_ref[:, : 128 * cols], img_b[...], 0, 0
    )
    for k, ref in enumerate(out_refs):
        part, at = (image_part, k) if k < rows else (text_part, k - rows)
        ref[...] = part[128 * at : 128 * at + 128, :].astype(ref.dtype)


def shape(*dims, dtype=jnp.float32):
    return jax.ShapeDtypeStruct(dims, dtype)


def call(kernel, specs, outs, flops):
    return pl.pallas_call(
        kernel,
        in_specs=specs,
        out_specs=[VMEM] * len(outs),
        out_shape=outs,
        compiler_params=PARAMS,
        cost_estimate=pl.CostEstimate(flops=flops, bytes_accessed=4 << 20, transcendentals=1 << 20),
    )


def merge_lse(first, second):
    top = jnp.maximum(first, second)
    return top + jnp.log(jnp.exp(first - top) + jnp.exp(second - top))


def step(images, texts, scale, cotangent):
    n, width = images.shape
    logit_scale = scale[0]
    at_z, at_x, at_h = (lax.axis_index(a) for a in ("z", "x", "h"))
    z_n, x_n = lax.axis_size("z"), lax.axis_size("x")
    c_n = 2 * x_n
    half = z_n // 2
    offs = [0] + [s * k for k in range(1, half) for s in (1, -1)] + [half]
    turns = [(d, e) for d in (0, 1, 3, 2) for e in (0, 1)]
    img_held = gather_z(images)
    txt_held = gather_xh(texts)
    rows_a, cols = (z_n - 1) * n, c_n * n
    tile = 2 * cols * width * n
    s_a, row_a, top_a, sum_a, img_a, txt = call(
        functools.partial(stats_a_kernel, z_n - 1),
        [SMEM] + [VMEM] * (z_n - 1 + c_n),
        [shape(rows_a, cols), shape(z_n - 1, n), shape(1, cols), shape(1, cols)]
        + [shape(r, width, dtype=jnp.bfloat16) for r in (rows_a, cols)],
        7 * tile,
    )(scale, *[img_held[o] for o in offs[:-1]], *[txt_held[t] for t in turns])
    img_b = img_held[half]
    s_b, row_b, col_part = call(
        stats_b_kernel, [SMEM] + [VMEM] * 4, [shape(n, cols), shape(1, n), shape(c_n, n)], tile
    )(scale, img_b, txt, top_a, sum_a)
    row_part = jnp.concatenate([row_a, row_b], axis=0)

    z_ids = jnp.stack([(at_z + o) % z_n for o in offs])
    c_ids = jnp.stack([((at_x + d) % x_n) * 2 + (at_h ^ e) for d, e in turns])
    z_hot = (z_ids[:, None] == jnp.arange(z_n)[None, :])[:, :, None]
    c_hot = (c_ids[:, None] == jnp.arange(c_n)[None, :])[:, :, None]

    def placed(value, hot, cot):
        spread = jnp.sum(jnp.where(hot, value[:, None, :], 0.0), axis=0)
        return jnp.concatenate([spread, jnp.where(hot[0], cot, 0.0)], axis=0)

    def taken(value, hot):
        count = hot.shape[1]
        halves = value.reshape(2, 1, count, n)
        return jnp.sum(jnp.where(hot[None], halves, 0.0), axis=2).reshape(2 * count, n)

    def merged(mine, got, count):
        return jnp.concatenate(
            [merge_lse(mine[:count], got[:count]), mine[count:] + got[count:]], axis=0
        )

    row_msg = placed(row_part, z_hot, cotangent[:1])
    col_msg = placed(col_part, c_hot, cotangent[1:])
    for z_bit, col_axis, col_bit in ((1, "h", 1), (2, "x", 1), (4, "x", 2)):
        row_got = swapped(row_msg, "z", z_bit)
        col_got = swapped(col_msg, col_axis, col_bit)
        row_msg = merged(row_msg, row_got, z_n)
        col_msg = merged(col_msg, col_got, c_n)
    row_all = taken(row_msg, z_hot)
    col_all = taken(col_msg, c_hot)

    sent = shape(n, width, dtype=jnp.bfloat16)
    kept = shape(n, width)
    w_a, w_b, down_msg, up, fore, back = call(
        weights_kernel,
        [VMEM] * 7,
        [shape(r, cols, dtype=jnp.bfloat16) for r in (rows_a, n)] + [sent] * 4,
        4 * tile,
    )(s_a, s_b, row_all, col_all, img_a, img_b, txt)
    direct = ((1, 1), (3, 0))
    parts = call(
        functools.partial(rest_kernel, z_n - 2, c_n - 2),
        [VMEM] * 5,
        [kept] * (z_n - 2) + [sent if t in direct else kept for t in turns[:-2]],
        12 * tile,
    )(w_a, w_b, img_a, img_b, txt)
    part = dict(zip(offs[:-2], parts[: z_n - 2]))
    piece = dict(zip(turns[:-2], parts[z_n - 2 :]))

    up = moved(up, "z", 1)
    down_msg = moved(down_msg, "z", -1)
    for k in range(half - 1, 0, -1):
        up = moved(low(part[k] + wide(up)), "z", 1)
        if k < half - 1:
            down_msg = moved(low(part[-k] + wide(down_msg)), "z", -1)
    img_terms = part[0] + wide(up) + wide(down_msg)

    fore = moved(fore, "x", 1)
    back = moved(back, "x", -1)
    fore1 = moved(piece[1, 1], "x", 1)
    back0 = moved(piece[3, 0], "x", -1)
    fore0 = moved(low(piece[1, 0] + wide(fore)), "x", 1)
    back1 = moved(low(piece[3, 1] + wide(back)), "x", -1)
    other = moved(low(piece[0, 1] + wide(fore1) + wide(back1)), "h", 1)
    txt_terms = piece[0, 0] + wide(fore0) + wide(back0) + wide(other)

    matched = logit_scale * jnp.sum(wide(images) * wide(texts), axis=1)
    row_losses = jnp.stack([row_all[0] - matched, col_all[0] - matched])
    both_cot = (cotangent[0] + cotangent[1])[:, None]
    grad_images = logit_scale * (img_terms - both_cot * wide(texts))
    grad_texts = logit_scale * (txt_terms - both_cot * wide(images))
    return (row_losses, grad_images, grad_texts)


def solution(mesh):
    grid = Mesh(mesh.devices.reshape(4, 8, 2, 4), ("x", "z", "h", "dp"))
    rows = ("dp", "x", "z", "h")
    return jax.shard_map(
        step,
        mesh=grid,
        in_specs=(P(rows, None), P(rows, None), P(), P(None, rows)),
        out_specs=(P(None, rows), P(rows, None), P(rows, None)),
        check_vma=False,
    )
```

```python
import functools

import jax
import jax.numpy as jnp
from jax import lax
from jax.experimental import pallas as pl
from jax.experimental.pallas import tpu as pltpu
from jax.sharding import Mesh, PartitionSpec as P

VMEM = pl.BlockSpec(memory_space=pltpu.VMEM)
SMEM = pl.BlockSpec(memory_space=pltpu.SMEM)
PARAMS = pltpu.CompilerParams(vmem_limit_bytes=24 * 1024 * 1024)


def moved(value, axis, steps):
    count = lax.axis_size(axis)
    return lax.ppermute(value, axis, [(i, (i + steps) % count) for i in range(count)])


def swapped(value, axis, bit):
    count = lax.axis_size(axis)
    return lax.ppermute(value, axis, [(i, i ^ bit) for i in range(count)])


def gather_z(block):
    half = lax.axis_size("z") // 2
    held = {0: block}
    for k in range(1, half):
        held[-k] = moved(held[1 - k], "z", 1)
        held[k] = moved(held[k - 1], "z", -1)
    held[half] = moved(held[half - 2], "z", -2)
    return held


def gather_xh(block):
    held = {(0, 0): block, (0, 1): moved(block, "h", 1)}
    for e in (0, 1):
        held[1, e] = moved(held[0, e], "x", -1)
        held[3, e] = moved(held[0, e], "x", 1)
    held[2, 0] = moved(held[1, 0], "x", -1)
    held[2, 1] = moved(held[3, 1], "x", 1)
    return held


def low(value):
    return value.astype(jnp.bfloat16)


def wide(value):
    return value.astype(jnp.float32)


def across(column):
    return jnp.broadcast_to(column, (column.shape[0], 128)).T[0:1, :]


def down(row):
    return jnp.broadcast_to(row, (128, row.shape[1])).T


def product(left, right, left_dim, right_dim):
    return lax.dot_general(
        left, right, (((left_dim,), (right_dim,)), ((), ())), preferred_element_type=jnp.float32
    )


def stage_kernel(scale_ref, cot_ref, img_in, txt_in, img_ref, txt_ref, gi_ref, gt_ref, match_ref):
    img, txt = wide(img_in[...]), wide(txt_in[...])
    img_ref[...] = img_in[...]
    txt_ref[...] = txt_in[...]
    both = down(cot_ref[0:1, :] + cot_ref[1:2, :])[:, 0:1]
    gi_ref[...] = both * txt
    gt_ref[...] = both * img
    match_ref[...] = across(scale_ref[0] * jnp.sum(img * txt, axis=1, keepdims=True))


def scores_into(scale_ref, img_ref, txt_ref, s_ref):
    for c in range(0, txt_ref.shape[0], 256):
        part = product(img_ref[...], txt_ref[c : c + 256, :], 1, 1)
        s_ref[:, c : c + 256] = scale_ref[0] * part
    return jnp.max(s_ref[...], axis=0, keepdims=True)


def stats_into(s_ref, row_ref, col_top):
    col_sum = jnp.zeros_like(col_top)
    for b in range(row_ref.shape[0]):
        s = s_ref[128 * b : 128 * b + 128, :]
        top = jnp.max(s, axis=1, keepdims=True)
        total = jnp.sum(jnp.exp(s - top), axis=1, keepdims=True)
        row_ref[b : b + 1, :] = across(top + jnp.log(total))
        col_sum = col_sum + jnp.sum(jnp.exp(s - col_top), axis=0, keepdims=True)
    return col_sum


def pack(refs, into):
    for b, ref in enumerate(refs):
        into[128 * b : 128 * b + 128, :] = ref[...]


def stats_a_kernel(blocks, scale_ref, *refs):
    s_ref, row_ref, top_ref, sum_ref, img_ref, txt_ref = refs[-6:]
    pack(refs[:blocks], img_ref)
    pack(refs[blocks:-6], txt_ref)
    col_top = scores_into(scale_ref, img_ref, txt_ref, s_ref)
    top_ref[...] = col_top
    sum_ref[...] = stats_into(s_ref, row_ref, col_top)


def stats_b_kernel(blocks, scale_ref, *refs):
    txt_ref, top_ref, sum_ref, s_ref, row_ref, col_ref, img_ref = refs[blocks:]
    pack(refs[:blocks], img_ref)
    col_top = jnp.maximum(scores_into(scale_ref, img_ref, txt_ref, s_ref), top_ref[...])
    col_sum = stats_into(s_ref, row_ref, col_top) + sum_ref[...] * jnp.exp(top_ref[...] - col_top)
    lse = col_top + jnp.log(col_sum)
    for c in range(0, lse.shape[1], 128):
        col_ref[c // 128 : c // 128 + 1, :] = lse[:, c : c + 128]


def weights_into(s_ref, w_ref, row_ref, col_ref, at):
    blocks = row_ref.shape[0] // 2
    cols = col_ref.shape[0] // 2
    for b in range(w_ref.shape[0] // 128):
        row_lse = down(row_ref[at + b : at + b + 1, :])
        row_cot = down(row_ref[blocks + at + b : blocks + at + b + 1, :])
        for c in range(cols):
            s = s_ref[128 * b : 128 * b + 128, 128 * c : 128 * c + 128]
            w = row_cot * jnp.exp(s - row_lse) + col_ref[cols + c : cols + c + 1, :] * jnp.exp(
                s - col_ref[c : c + 1, :]
            )
            w_ref[128 * b : 128 * b + 128, 128 * c : 128 * c + 128] = low(w)


def text_product(wa_ref, wb_ref, img_a, img_b, cols):
    return product(wa_ref[:, cols], img_a[...], 0, 0) + product(wb_ref[:, cols], img_b[...], 0, 0)


def weights_kernel(
    blocks, sa_ref, sb_ref, row_ref, col_ref, img_a, img_b, txt_ref, wa_ref, wb_ref, *out_refs
):
    weights_into(sb_ref, wb_ref, row_ref, col_ref, wa_ref.shape[0] // 128)
    image_part = product(wb_ref[...], txt_ref[...], 1, 0)
    for k in range(blocks):
        out_refs[k][...] = low(image_part[128 * k : 128 * k + 128, :])
    weights_into(sa_ref, wa_ref, row_ref, col_ref, 0)
    width = wa_ref.shape[1]
    text_part = text_product(wa_ref, wb_ref, img_a, img_b, slice(width - 256, width))
    for k in range(2):
        out_refs[blocks + k][...] = low(text_part[128 * k : 128 * k + 128, :])


def rest_kernel(rows, cols, wa_ref, wb_ref, img_a, img_b, txt_ref, gi_ref, gt_ref, *refs):
    match_ref, row_ref, col_ref = refs[:3]
    out_refs, loss_ref = refs[3:-1], refs[-1]
    image_part = product(wa_ref[...], txt_ref[...], 1, 0)
    out_refs[0][...] = image_part[:128, :] - gi_ref[...]
    for k in range(1, rows):
        out_refs[k][...] = image_part[128 * k : 128 * k + 128, :]
    text_part = text_product(wa_ref, wb_ref, img_a, img_b, slice(0, 128 * cols))
    out_refs[rows][...] = text_part[:128, :] - gt_ref[...]
    for k in range(1, cols):
        ref = out_refs[rows + k]
        ref[...] = text_part[128 * k : 128 * k + 128, :].astype(ref.dtype)
    loss_ref[0:1, :] = row_ref[0:1, :] - match_ref[...]
    loss_ref[1:2, :] = col_ref[0:1, :] - match_ref[...]


def shape(*dims, dtype=jnp.float32):
    return jax.ShapeDtypeStruct(dims, dtype)


def call(kernel, specs, outs, flops):
    return pl.pallas_call(
        kernel,
        in_specs=specs,
        out_specs=[VMEM] * len(outs),
        out_shape=outs,
        compiler_params=PARAMS,
        cost_estimate=pl.CostEstimate(flops=flops, bytes_accessed=4 << 20, transcendentals=1 << 20),
    )


def merge_lse(first, second):
    top = jnp.maximum(first, second)
    return top + jnp.log(jnp.exp(first - top) + jnp.exp(second - top))


def step(images, texts, scale, cotangent):
    n, width = images.shape
    logit_scale = scale[0]
    at_z, at_x, at_h = (lax.axis_index(a) for a in ("z", "x", "h"))
    z_n, x_n = lax.axis_size("z"), lax.axis_size("x")
    c_n = 2 * x_n
    half = z_n // 2
    offs = [0] + [s * k for k in range(1, half) for s in (1, -1)] + [half]
    turns = [(d, e) for d in (0, 1, 3, 2) for e in (0, 1)]
    cols = c_n * n
    early = half + 1
    late = z_n - early
    tile = 2 * cols * width * n
    sent = shape(n, width, dtype=jnp.bfloat16)
    kept = shape(n, width)
    img_held = gather_z(images)
    txt_held = gather_xh(texts)
    img_own, txt_own, base_i, base_t, matched = call(
        stage_kernel, [SMEM] + [VMEM] * 3, [sent, sent, kept, kept, shape(1, n)], tile // 8
    )(scale, cotangent, images, texts)
    img_held[0], txt_held[0, 0] = img_own, txt_own
    s_a, row_a, top_a, sum_a, img_a, txt = call(
        functools.partial(stats_a_kernel, early),
        [SMEM] + [VMEM] * (early + c_n),
        [shape(early * n, cols), shape(early, n), shape(1, cols), shape(1, cols)]
        + [shape(r, width, dtype=jnp.bfloat16) for r in (early * n, cols)],
        early * tile,
    )(scale, *[img_held[o] for o in offs[:early]], *[txt_held[t] for t in turns])
    s_b, row_b, col_part, img_b = call(
        functools.partial(stats_b_kernel, late),
        [SMEM] + [VMEM] * (late + 3),
        [shape(late * n, cols), shape(late, n), shape(c_n, n)]
        + [shape(late * n, width, dtype=jnp.bfloat16)],
        late * tile,
    )(scale, *[img_held[o] for o in offs[early:]], txt, top_a, sum_a)
    row_part = jnp.concatenate([row_a, row_b], axis=0)

    z_ids = jnp.stack([(at_z + o) % z_n for o in offs])
    c_ids = jnp.stack([((at_x + d) % x_n) * 2 + (at_h ^ e) for d, e in turns])
    z_hot = (z_ids[:, None] == jnp.arange(z_n)[None, :])[:, :, None]
    c_hot = (c_ids[:, None] == jnp.arange(c_n)[None, :])[:, :, None]

    def placed(value, hot, cot):
        spread = jnp.sum(jnp.where(hot, value[:, None, :], 0.0), axis=0)
        return jnp.concatenate([spread, jnp.where(hot[0], cot, 0.0)], axis=0)

    def taken(value, hot):
        count = hot.shape[1]
        halves = value.reshape(2, 1, count, n)
        return jnp.sum(jnp.where(hot[None], halves, 0.0), axis=2).reshape(2 * count, n)

    def merged(mine, got, count):
        return jnp.concatenate(
            [merge_lse(mine[:count], got[:count]), mine[count:] + got[count:]], axis=0
        )

    row_msg = placed(row_part, z_hot, cotangent[:1])
    col_msg = placed(col_part, c_hot, cotangent[1:])
    for z_bit, col_axis, col_bit in ((4, "h", 1), (2, "x", 2), (1, "x", 1)):
        row_got = swapped(row_msg, "z", z_bit)
        col_got = swapped(col_msg, col_axis, col_bit)
        row_msg = merged(row_msg, row_got, z_n)
        col_msg = merged(col_msg, col_got, c_n)
    row_all = taken(row_msg, z_hot)
    col_all = taken(col_msg, c_hot)

    w_a, w_b, up, down_msg, far, fore, back = call(
        functools.partial(weights_kernel, late),
        [VMEM] * 7,
        [shape(r * n, cols, dtype=jnp.bfloat16) for r in (early, late)] + [sent] * (late + 2),
        4 * tile,
    )(s_a, s_b, row_all, col_all, img_a, img_b, txt)
    direct = ((1, 1), (3, 0))
    parts = call(
        functools.partial(rest_kernel, early, c_n - 2),
        [VMEM] * 10,
        [kept] * early
        + [sent if t in direct else kept for t in turns[:-2]]
        + [shape(2, n)],
        12 * tile,
    )(w_a, w_b, img_a, img_b, txt, base_i, base_t, matched, row_all, col_all)
    part = dict(zip(offs[:early], parts[:early]))
    piece = dict(zip(turns[:-2], parts[early:-1]))

    far = wide(moved(far, "z", 2))
    up = moved(up, "z", 1)
    down_msg = moved(down_msg, "z", -1)
    for k in range(half - 2, 0, -1):
        total = part[k] + wide(up)
        if k == half - 2:
            total = total + far
        up = moved(low(total), "z", 1)
        down_msg = moved(low(part[-k] + wide(down_msg)), "z", -1)
    img_terms = part[0] + wide(up) + wide(down_msg)

    fore = moved(fore, "x", 1)
    back = moved(back, "x", -1)
    fore1 = moved(piece[1, 1], "x", 1)
    back0 = moved(piece[3, 0], "x", -1)
    fore0 = moved(low(piece[1, 0] + wide(fore)), "x", 1)
    back1 = moved(low(piece[3, 1] + wide(back)), "x", -1)
    other = moved(low(piece[0, 1] + wide(fore1) + wide(back1)), "h", 1)
    txt_terms = piece[0, 0] + wide(fore0) + wide(back0) + wide(other)

    return (parts[-1], logit_scale * img_terms, logit_scale * txt_terms)


def solution(mesh):
    grid = Mesh(mesh.devices.reshape(4, 8, 2, 4), ("x", "z", "h", "dp"))
    rows = ("dp", "x", "z", "h")
    return jax.shard_map(
        step,
        mesh=grid,
        in_specs=(P(rows, None), P(rows, None), P(), P(None, rows)),
        out_specs=(P(None, rows), P(rows, None), P(rows, None)),
        check_vma=False,
    )
```

```python
import functools

import jax
import jax.numpy as jnp
from jax import lax
from jax.experimental import pallas as pl
from jax.experimental.pallas import tpu as pltpu
from jax.sharding import Mesh, PartitionSpec as P

VMEM = pl.BlockSpec(memory_space=pltpu.VMEM)
SMEM = pl.BlockSpec(memory_space=pltpu.SMEM)
PARAMS = pltpu.CompilerParams(vmem_limit_bytes=24 * 1024 * 1024)


def moved(value, axis, steps):
    count, lanes = lax.axis_size(axis), lax.axis_size("dp")
    pairs = [
        (i * lanes + c, (i + (steps if c % 2 == 0 else -steps)) % count * lanes + c)
        for i in range(count)
        for c in range(lanes)
    ]
    return lax.ppermute(value, (axis, "dp"), pairs)


def swapped(value, axis, bit):
    count = lax.axis_size(axis)
    return lax.ppermute(value, axis, [(i, i ^ bit) for i in range(count)])


def gather_z(block):
    half = lax.axis_size("z") // 2
    held = {0: block}
    for k in range(1, half):
        held[-k] = moved(held[1 - k], "z", 1)
        held[k] = moved(held[k - 1], "z", -1)
    held[half] = moved(held[half - 2], "z", -2)
    return held


def gather_xh(block, own):
    other = moved(block, "h", 1)
    near = [moved(block, "x", -1), moved(other, "x", -1)]
    back = moved(jnp.concatenate([own, other], axis=0), "x", 1)
    far = moved(jnp.concatenate(near, axis=0), "x", -1)
    return [own, other, *near, back, far]


def low(value):
    return value.astype(jnp.bfloat16)


def wide(value):
    return value.astype(jnp.float32)


def across(column):
    return jnp.broadcast_to(column, (column.shape[0], 128)).T[0:1, :]


def down(row):
    return jnp.broadcast_to(row, (128, row.shape[1])).T


def product(left, right, left_dim, right_dim):
    return lax.dot_general(
        left, right, (((left_dim,), (right_dim,)), ((), ())), preferred_element_type=jnp.float32
    )


def stage_kernel(scale_ref, cot_in, img_in, txt_in, *refs):
    cot_ref, img_ref, txt_ref, gi_ref, gt_ref, match_ref, sems = refs
    copies = [
        pltpu.make_async_copy(source, target, sems.at[k])
        for k, (source, target) in enumerate(
            ((img_in, img_ref), (txt_in, txt_ref), (cot_in, cot_ref))
        )
    ]
    for copy in copies:
        copy.start()
    for copy in copies:
        copy.wait()
    img, txt = wide(img_ref[...]), wide(txt_ref[...])
    both = down(cot_ref[0:1, :] + cot_ref[1:2, :])[:, 0:1]
    gi_ref[...] = both * txt
    gt_ref[...] = both * img
    match_ref[...] = across(scale_ref[0] * jnp.sum(img * txt, axis=1, keepdims=True))


def scores_into(scale_ref, img_ref, txt_ref, s_ref):
    for c in range(0, txt_ref.shape[0], 256):
        part = product(img_ref[...], txt_ref[c : c + 256, :], 1, 1)
        s_ref[:, c : c + 256] = scale_ref[0] * part
    return jnp.max(s_ref[...], axis=0, keepdims=True)


def stats_into(s_ref, row_ref, col_top):
    col_sum = jnp.zeros_like(col_top)
    for b in range(row_ref.shape[0]):
        s = s_ref[128 * b : 128 * b + 128, :]
        top = jnp.max(s, axis=1, keepdims=True)
        total = jnp.sum(jnp.exp(s - top), axis=1, keepdims=True)
        row_ref[b : b + 1, :] = across(top + jnp.log(total))
        col_sum = col_sum + jnp.sum(jnp.exp(s - col_top), axis=0, keepdims=True)
    return col_sum


def pack(refs, into):
    at = 0
    for ref in refs:
        into[at : at + ref.shape[0], :] = ref[...]
        at += ref.shape[0]


def stats_a_kernel(blocks, scale_ref, *refs):
    s_ref, row_ref, top_ref, sum_ref, img_ref, txt_ref = refs[-6:]
    pack(refs[:blocks], img_ref)
    pack(refs[blocks:-6], txt_ref)
    col_top = scores_into(scale_ref, img_ref, txt_ref, s_ref)
    top_ref[...] = col_top
    sum_ref[...] = stats_into(s_ref, row_ref, col_top)


def stats_b_kernel(blocks, scale_ref, *refs):
    txt_ref, top_ref, sum_ref, s_ref, row_ref, col_ref, img_ref = refs[blocks:]
    pack(refs[:blocks], img_ref)
    col_top = jnp.maximum(scores_into(scale_ref, img_ref, txt_ref, s_ref), top_ref[...])
    col_sum = stats_into(s_ref, row_ref, col_top) + sum_ref[...] * jnp.exp(top_ref[...] - col_top)
    lse = col_top + jnp.log(col_sum)
    for c in range(0, lse.shape[1], 128):
        col_ref[c // 128 : c // 128 + 1, :] = lse[:, c : c + 128]


def weights_into(s_ref, w_ref, row_ref, col_ref, at):
    blocks = row_ref.shape[0] // 2
    cols = col_ref.shape[0] // 2
    for b in range(w_ref.shape[0] // 128):
        row_lse = down(row_ref[at + b : at + b + 1, :])
        row_cot = down(row_ref[blocks + at + b : blocks + at + b + 1, :])
        for c in range(cols):
            s = s_ref[128 * b : 128 * b + 128, 128 * c : 128 * c + 128]
            w = row_cot * jnp.exp(s - row_lse) + col_ref[cols + c : cols + c + 1, :] * jnp.exp(
                s - col_ref[c : c + 1, :]
            )
            w_ref[128 * b : 128 * b + 128, 128 * c : 128 * c + 128] = low(w)


def text_product(wa_ref, wb_ref, img_a, img_b, cols):
    return product(wa_ref[:, cols], img_a[...], 0, 0) + product(wb_ref[:, cols], img_b[...], 0, 0)


def weights_kernel(
    blocks, sa_ref, sb_ref, row_ref, col_ref, img_a, img_b, txt_ref, wa_ref, wb_ref, *out_refs
):
    weights_into(sb_ref, wb_ref, row_ref, col_ref, wa_ref.shape[0] // 128)
    image_part = product(wb_ref[...], txt_ref[...], 1, 0)
    for k in range(blocks):
        out_refs[k][...] = low(image_part[128 * k : 128 * k + 128, :])
    weights_into(sa_ref, wa_ref, row_ref, col_ref, 0)
    width = wa_ref.shape[1]
    text_part = text_product(wa_ref, wb_ref, img_a, img_b, slice(width - 512, width))
    for k in range(2):
        out_refs[blocks + k][...] = low(text_part[256 * k : 256 * k + 256, :])


def rest_kernel(wa_ref, wb_ref, img_a, img_b, txt_ref, gi_ref, gt_ref, *refs):
    match_ref, row_ref, col_ref = refs[:3]
    *image_refs, text_ref, loss_ref = refs[3:]
    text_ref[...] = text_product(wa_ref, wb_ref, img_a, img_b, slice(0, text_ref.shape[0]))
    text_ref[:128, :] = text_ref[:128, :] - gt_ref[...]
    image_part = product(wa_ref[...], txt_ref[...], 1, 0)
    image_refs[0][...] = image_part[:128, :] - gi_ref[...]
    for k in range(1, len(image_refs)):
        image_refs[k][...] = image_part[128 * k : 128 * k + 128, :]
    loss_ref[0:1, :] = row_ref[0:1, :] - match_ref[...]
    loss_ref[1:2, :] = col_ref[0:1, :] - match_ref[...]


def shape(*dims, dtype=jnp.float32):
    return jax.ShapeDtypeStruct(dims, dtype)


def call(kernel, specs, outs, flops, scratch=()):
    return pl.pallas_call(
        kernel,
        in_specs=specs,
        out_specs=[VMEM] * len(outs),
        out_shape=outs,
        scratch_shapes=scratch,
        compiler_params=PARAMS,
        cost_estimate=pl.CostEstimate(flops=flops, bytes_accessed=4 << 20, transcendentals=1 << 20),
    )


def merge_lse(first, second):
    top = jnp.maximum(first, second)
    return top + jnp.log(jnp.exp(first - top) + jnp.exp(second - top))


def step(images, texts, scale, cotangent):
    n, width = images.shape
    logit_scale = scale[0]
    at_z, at_x, at_h = (lax.axis_index(a) for a in ("z", "x", "h"))
    z_n, x_n = lax.axis_size("z"), lax.axis_size("x")
    c_n = 2 * x_n
    half = z_n // 2
    offs = [0] + [s * k for k in range(1, half) for s in (1, -1)] + [half]
    turns = [(d, e) for d in (0, 1, -1, 2) for e in (0, 1)]
    cols = c_n * n
    early = half + 1
    late = z_n - early
    tile = 2 * cols * width * n
    sent = shape(n, width, dtype=jnp.bfloat16)
    kept = shape(n, width)
    img_held = gather_z(images)
    cot, img_own, txt_own, base_i, base_t, matched = call(
        stage_kernel,
        [SMEM] + [pl.BlockSpec(memory_space=pltpu.HBM)] * 3,
        [shape(2, n), sent, sent, kept, kept, shape(1, n)],
        tile // 8,
        [pltpu.SemaphoreType.DMA((3,))],
    )(scale, *[pltpu.with_memory_space_constraint(v, pltpu.HBM) for v in (cotangent, images, texts)])
    img_held[0] = img_own
    txt_held = gather_xh(texts, txt_own)
    s_a, row_a, top_a, sum_a, img_a, txt = call(
        functools.partial(stats_a_kernel, early),
        [SMEM] + [VMEM] * (early + len(txt_held)),
        [shape(early * n, cols), shape(early, n), shape(1, cols), shape(1, cols)]
        + [shape(r, width, dtype=jnp.bfloat16) for r in (early * n, cols)],
        early * tile,
    )(scale, *[img_held[o] for o in offs[:early]], *txt_held)
    s_b, row_b, col_part, img_b = call(
        functools.partial(stats_b_kernel, late),
        [SMEM] + [VMEM] * (late + 3),
        [shape(late * n, cols), shape(late, n), shape(c_n, n)]
        + [shape(late * n, width, dtype=jnp.bfloat16)],
        late * tile,
    )(scale, *[img_held[o] for o in offs[early:]], txt, top_a, sum_a)
    row_part = jnp.concatenate([row_a, row_b], axis=0)

    turn = 1 - 2 * (lax.axis_index("dp") % 2)
    z_ids = jnp.stack([(at_z + o * turn) % z_n for o in offs])
    c_ids = jnp.stack([((at_x + d * turn) % x_n) * 2 + (at_h ^ e) for d, e in turns])
    z_hot = (z_ids[:, None] == jnp.arange(z_n)[None, :])[:, :, None]
    c_hot = (c_ids[:, None] == jnp.arange(c_n)[None, :])[:, :, None]

    def placed(value, hot, cot):
        spread = jnp.sum(jnp.where(hot, value[:, None, :], 0.0), axis=0)
        return jnp.concatenate([spread, jnp.where(hot[0], cot, 0.0)], axis=0)

    def taken(value, hot):
        count = hot.shape[1]
        halves = value.reshape(2, 1, count, n)
        return jnp.sum(jnp.where(hot[None], halves, 0.0), axis=2).reshape(2 * count, n)

    def merged(mine, got, count):
        return jnp.concatenate(
            [merge_lse(mine[:count], got[:count]), mine[count:] + got[count:]], axis=0
        )

    row_msg = placed(row_part, z_hot, cot[:1])
    col_msg = placed(col_part, c_hot, cot[1:])
    for z_bit, col_axis, col_bit in ((4, "h", 1), (2, "x", 2), (1, "x", 1)):
        row_got = swapped(row_msg, "z", z_bit)
        col_got = swapped(col_msg, col_axis, col_bit)
        row_msg = merged(row_msg, row_got, z_n)
        col_msg = merged(col_msg, col_got, c_n)
    row_all = taken(row_msg, z_hot)
    col_all = taken(col_msg, c_hot)

    pair = shape(2 * n, width, dtype=jnp.bfloat16)
    w_a, w_b, up, down_msg, far, back, far_x = call(
        functools.partial(weights_kernel, late),
        [VMEM] * 7,
        [shape(r * n, cols, dtype=jnp.bfloat16) for r in (early, late)]
        + [sent] * late
        + [pair] * 2,
        5 * tile,
    )(s_a, s_b, row_all, col_all, img_a, img_b, txt)
    *parts, piece, row_losses = call(
        rest_kernel, [VMEM] * 10, [kept] * early + [shape(4 * n, width), shape(2, n)], 9 * tile
    )(w_a, w_b, img_a, img_b, txt, base_i, base_t, matched, row_all, col_all)
    part = dict(zip(offs[:early], parts))

    far = wide(moved(far, "z", 2))
    up = moved(up, "z", 1)
    down_msg = moved(down_msg, "z", -1)
    for k in range(half - 2, 0, -1):
        total = part[k] + wide(up)
        if k == half - 2:
            total = total + far
        up = moved(low(total), "z", 1)
        down_msg = moved(low(part[-k] + wide(down_msg)), "z", -1)
    img_terms = part[0] + wide(up) + wide(down_msg)

    far_x = moved(far_x, "x", 1)
    back = wide(moved(back, "x", -1))
    near = wide(moved(low(piece[2 * n :] + wide(far_x)), "x", 1))
    other = wide(moved(low(piece[n : 2 * n] + near[n:] + back[n:]), "h", 1))
    grad_texts = logit_scale * (piece[:n] + near[:n] + back[:n] + other)
    return (row_losses, logit_scale * img_terms, grad_texts)


def solution(mesh):
    grid = Mesh(mesh.devices.reshape(4, 8, 2, 4), ("x", "z", "h", "dp"))
    rows = ("dp", "x", "z", "h")
    return jax.shard_map(
        step,
        mesh=grid,
        in_specs=(P(rows, None), P(rows, None), P(), P(None, rows)),
        out_specs=(P(None, rows), P(rows, None), P(rows, None)),
        check_vma=False,
    )
```

```python
import functools

import jax
import jax.numpy as jnp
from jax import lax
from jax.experimental import pallas as pl
from jax.experimental.pallas import tpu as pltpu
from jax.sharding import Mesh, PartitionSpec as P

VMEM = pl.BlockSpec(memory_space=pltpu.VMEM)
SMEM = pl.BlockSpec(memory_space=pltpu.SMEM)
PARAMS = pltpu.CompilerParams(vmem_limit_bytes=24 * 1024 * 1024)


def moved(value, axis, steps):
    count, lanes = lax.axis_size(axis), lax.axis_size("dp")
    pairs = [
        (i * lanes + c, (i + (steps if c % 2 == 0 else -steps)) % count * lanes + c)
        for i in range(count)
        for c in range(lanes)
    ]
    return lax.ppermute(value, (axis, "dp"), pairs)


def swapped(value, axis, bit):
    count = lax.axis_size(axis)
    return lax.ppermute(value, axis, [(i, i ^ bit) for i in range(count)])


def gather_z(block):
    half = lax.axis_size("z") // 2
    held = {0: block}
    for k in range(1, half):
        held[-k] = moved(held[1 - k], "z", 1)
        held[k] = moved(held[k - 1], "z", -1)
    held[half] = moved(held[half - 2], "z", -2)
    return held


def gather_xh(block):
    held = {(0, 0): block, (0, 1): moved(block, "h", 1)}
    for e in (0, 1):
        held[1, e] = moved(held[0, e], "x", -1)
        held[3, e] = moved(held[0, e], "x", 1)
    held[2, 0] = moved(held[1, 0], "x", -1)
    held[2, 1] = moved(held[3, 1], "x", 1)
    return held


def low(value):
    return value.astype(jnp.bfloat16)


def wide(value):
    return value.astype(jnp.float32)


def across(column):
    return jnp.broadcast_to(column, (column.shape[0], 128)).T[0:1, :]


def down(row):
    return jnp.broadcast_to(row, (128, row.shape[1])).T


def product(left, right, left_dim, right_dim):
    return lax.dot_general(
        left, right, (((left_dim,), (right_dim,)), ((), ())), preferred_element_type=jnp.float32
    )


def stage_kernel(scale_ref, cot_in, img_in, txt_in, *refs):
    cot_ref, img_ref, txt_ref, gi_ref, gt_ref, match_ref, sems = refs
    copies = [
        pltpu.make_async_copy(source, target, sems.at[k])
        for k, (source, target) in enumerate(
            ((img_in, img_ref), (txt_in, txt_ref), (cot_in, cot_ref))
        )
    ]
    for copy in copies:
        copy.start()
    for copy in copies:
        copy.wait()
    img, txt = wide(img_ref[...]), wide(txt_ref[...])
    both = down(cot_ref[0:1, :] + cot_ref[1:2, :])[:, 0:1]
    gi_ref[...] = both * txt
    gt_ref[...] = both * img
    match_ref[...] = across(scale_ref[0] * jnp.sum(img * txt, axis=1, keepdims=True))


def scores_into(scale_ref, img_ref, txt_ref, s_ref):
    for c in range(0, txt_ref.shape[0], 256):
        part = product(img_ref[...], txt_ref[c : c + 256, :], 1, 1)
        s_ref[:, c : c + 256] = scale_ref[0] * part
    return jnp.max(s_ref[...], axis=0, keepdims=True)


def stats_into(s_ref, row_ref, col_top):
    col_sum = jnp.zeros_like(col_top)
    for b in range(row_ref.shape[0]):
        s = s_ref[128 * b : 128 * b + 128, :]
        top = jnp.max(s, axis=1, keepdims=True)
        total = jnp.sum(jnp.exp(s - top), axis=1, keepdims=True)
        row_ref[b : b + 1, :] = across(top + jnp.log(total))
        col_sum = col_sum + jnp.sum(jnp.exp(s - col_top), axis=0, keepdims=True)
    return col_sum


def pack(refs, into):
    for b, ref in enumerate(refs):
        into[128 * b : 128 * b + 128, :] = ref[...]


def stats_a_kernel(blocks, scale_ref, *refs):
    s_ref, row_ref, top_ref, sum_ref, img_ref, txt_ref = refs[-6:]
    pack(refs[:blocks], img_ref)
    pack(refs[blocks:-6], txt_ref)
    col_top = scores_into(scale_ref, img_ref, txt_ref, s_ref)
    top_ref[...] = col_top
    sum_ref[...] = stats_into(s_ref, row_ref, col_top)


def stats_b_kernel(blocks, scale_ref, *refs):
    txt_ref, top_ref, sum_ref, s_ref, row_ref, col_ref, img_ref = refs[blocks:]
    pack(refs[:blocks], img_ref)
    col_top = jnp.maximum(scores_into(scale_ref, img_ref, txt_ref, s_ref), top_ref[...])
    col_sum = stats_into(s_ref, row_ref, col_top) + sum_ref[...] * jnp.exp(top_ref[...] - col_top)
    lse = col_top + jnp.log(col_sum)
    for c in range(0, lse.shape[1], 128):
        col_ref[c // 128 : c // 128 + 1, :] = lse[:, c : c + 128]


def weights_into(s_ref, w_ref, row_ref, col_ref, at):
    blocks = row_ref.shape[0] // 2
    cols = col_ref.shape[0] // 2
    for b in range(w_ref.shape[0] // 128):
        row_lse = down(row_ref[at + b : at + b + 1, :])
        row_cot = down(row_ref[blocks + at + b : blocks + at + b + 1, :])
        for c in range(cols):
            s = s_ref[128 * b : 128 * b + 128, 128 * c : 128 * c + 128]
            w = row_cot * jnp.exp(s - row_lse) + col_ref[cols + c : cols + c + 1, :] * jnp.exp(
                s - col_ref[c : c + 1, :]
            )
            w_ref[128 * b : 128 * b + 128, 128 * c : 128 * c + 128] = low(w)


def text_product(wa_ref, wb_ref, img_a, img_b, cols):
    return product(wa_ref[:, cols], img_a[...], 0, 0) + product(wb_ref[:, cols], img_b[...], 0, 0)


def weights_kernel(
    blocks, sa_ref, sb_ref, row_ref, col_ref, img_a, img_b, txt_ref, wa_ref, wb_ref, *out_refs
):
    weights_into(sb_ref, wb_ref, row_ref, col_ref, wa_ref.shape[0] // 128)
    image_part = product(wb_ref[...], txt_ref[...], 1, 0)
    for k in range(blocks):
        out_refs[k][...] = low(image_part[128 * k : 128 * k + 128, :])
    weights_into(sa_ref, wa_ref, row_ref, col_ref, 0)
    width = wa_ref.shape[1]
    text_part = text_product(wa_ref, wb_ref, img_a, img_b, slice(width - 256, width))
    for k in range(2):
        out_refs[blocks + k][...] = low(text_part[128 * k : 128 * k + 128, :])


def rest_kernel(rows, cols, wa_ref, wb_ref, img_a, img_b, txt_ref, gi_ref, gt_ref, *refs):
    match_ref, row_ref, col_ref = refs[:3]
    out_refs, loss_ref = refs[3:-1], refs[-1]
    image_part = product(wa_ref[...], txt_ref[...], 1, 0)
    out_refs[0][...] = image_part[:128, :] - gi_ref[...]
    for k in range(1, rows):
        out_refs[k][...] = image_part[128 * k : 128 * k + 128, :]
    text_part = text_product(wa_ref, wb_ref, img_a, img_b, slice(0, 128 * cols))
    out_refs[rows][...] = text_part[:128, :] - gt_ref[...]
    for k in range(1, cols):
        ref = out_refs[rows + k]
        ref[...] = text_part[128 * k : 128 * k + 128, :].astype(ref.dtype)
    loss_ref[0:1, :] = row_ref[0:1, :] - match_ref[...]
    loss_ref[1:2, :] = col_ref[0:1, :] - match_ref[...]


def shape(*dims, dtype=jnp.float32):
    return jax.ShapeDtypeStruct(dims, dtype)


def call(kernel, specs, outs, flops, scratch=()):
    return pl.pallas_call(
        kernel,
        in_specs=specs,
        out_specs=[VMEM] * len(outs),
        out_shape=outs,
        scratch_shapes=scratch,
        compiler_params=PARAMS,
        cost_estimate=pl.CostEstimate(flops=flops, bytes_accessed=4 << 20, transcendentals=1 << 20),
    )


def merge_lse(first, second):
    top = jnp.maximum(first, second)
    return top + jnp.log(jnp.exp(first - top) + jnp.exp(second - top))


def step(images, texts, scale, cotangent):
    n, width = images.shape
    logit_scale = scale[0]
    at_z, at_x, at_h = (lax.axis_index(a) for a in ("z", "x", "h"))
    z_n, x_n = lax.axis_size("z"), lax.axis_size("x")
    c_n = 2 * x_n
    half = z_n // 2
    offs = [0] + [s * k for k in range(1, half) for s in (1, -1)] + [half]
    turns = [(d, e) for d in (0, 1, 3, 2) for e in (0, 1)]
    cols = c_n * n
    early = half + 1
    late = z_n - early
    tile = 2 * cols * width * n
    sent = shape(n, width, dtype=jnp.bfloat16)
    kept = shape(n, width)
    img_held = gather_z(images)
    txt_held = gather_xh(texts)
    cot, img_own, txt_own, base_i, base_t, matched = call(
        stage_kernel,
        [SMEM] + [pl.BlockSpec(memory_space=pltpu.HBM)] * 3,
        [shape(2, n), sent, sent, kept, kept, shape(1, n)],
        tile // 8,
        [pltpu.SemaphoreType.DMA((3,))],
    )(scale, *[pltpu.with_memory_space_constraint(v, pltpu.HBM) for v in (cotangent, images, texts)])
    img_held[0], txt_held[0, 0] = img_own, txt_own
    s_a, row_a, top_a, sum_a, img_a, txt = call(
        functools.partial(stats_a_kernel, early),
        [SMEM] + [VMEM] * (early + c_n),
        [shape(early * n, cols), shape(early, n), shape(1, cols), shape(1, cols)]
        + [shape(r, width, dtype=jnp.bfloat16) for r in (early * n, cols)],
        early * tile,
    )(scale, *[img_held[o] for o in offs[:early]], *[txt_held[t] for t in turns])
    s_b, row_b, col_part, img_b = call(
        functools.partial(stats_b_kernel, late),
        [SMEM] + [VMEM] * (late + 3),
        [shape(late * n, cols), shape(late, n), shape(c_n, n)]
        + [shape(late * n, width, dtype=jnp.bfloat16)],
        late * tile,
    )(scale, *[img_held[o] for o in offs[early:]], txt, top_a, sum_a)
    row_part = jnp.concatenate([row_a, row_b], axis=0)

    turn = 1 - 2 * (lax.axis_index("dp") % 2)
    z_ids = jnp.stack([(at_z + o * turn) % z_n for o in offs])
    c_ids = jnp.stack([((at_x + d * turn) % x_n) * 2 + (at_h ^ e) for d, e in turns])
    z_hot = (z_ids[:, None] == jnp.arange(z_n)[None, :])[:, :, None]
    c_hot = (c_ids[:, None] == jnp.arange(c_n)[None, :])[:, :, None]

    def placed(value, hot, cot):
        spread = jnp.sum(jnp.where(hot, value[:, None, :], 0.0), axis=0)
        return jnp.concatenate([spread, jnp.where(hot[0], cot, 0.0)], axis=0)

    def taken(value, hot):
        count = hot.shape[1]
        halves = value.reshape(2, 1, count, n)
        return jnp.sum(jnp.where(hot[None], halves, 0.0), axis=2).reshape(2 * count, n)

    def merged(mine, got, count):
        return jnp.concatenate(
            [merge_lse(mine[:count], got[:count]), mine[count:] + got[count:]], axis=0
        )

    row_msg = placed(row_part, z_hot, cot[:1])
    col_msg = placed(col_part, c_hot, cot[1:])
    for z_bit, col_axis, col_bit in ((4, "h", 1), (2, "x", 2), (1, "x", 1)):
        row_got = swapped(row_msg, "z", z_bit)
        col_got = swapped(col_msg, col_axis, col_bit)
        row_msg = merged(row_msg, row_got, z_n)
        col_msg = merged(col_msg, col_got, c_n)
    row_all = taken(row_msg, z_hot)
    col_all = taken(col_msg, c_hot)

    w_a, w_b, up, down_msg, far, fore, back = call(
        functools.partial(weights_kernel, late),
        [VMEM] * 7,
        [shape(r * n, cols, dtype=jnp.bfloat16) for r in (early, late)] + [sent] * (late + 2),
        4 * tile,
    )(s_a, s_b, row_all, col_all, img_a, img_b, txt)
    direct = ((1, 1), (3, 0))
    parts = call(
        functools.partial(rest_kernel, early, c_n - 2),
        [VMEM] * 10,
        [kept] * early
        + [sent if t in direct else kept for t in turns[:-2]]
        + [shape(2, n)],
        12 * tile,
    )(w_a, w_b, img_a, img_b, txt, base_i, base_t, matched, row_all, col_all)
    part = dict(zip(offs[:early], parts[:early]))
    piece = dict(zip(turns[:-2], parts[early:-1]))

    far = wide(moved(far, "z", 2))
    up = moved(up, "z", 1)
    down_msg = moved(down_msg, "z", -1)
    for k in range(half - 2, 0, -1):
        total = part[k] + wide(up)
        if k == half - 2:
            total = total + far
        up = moved(low(total), "z", 1)
        down_msg = moved(low(part[-k] + wide(down_msg)), "z", -1)
    img_terms = part[0] + wide(up) + wide(down_msg)

    fore = moved(fore, "x", 1)
    back = moved(back, "x", -1)
    fore1 = moved(piece[1, 1], "x", 1)
    back0 = moved(piece[3, 0], "x", -1)
    fore0 = moved(low(piece[1, 0] + wide(fore)), "x", 1)
    back1 = moved(low(piece[3, 1] + wide(back)), "x", -1)
    other = moved(low(piece[0, 1] + wide(fore1) + wide(back1)), "h", 1)

    grad_texts = logit_scale * (piece[0, 0] + wide(fore0) + wide(back0) + wide(other))
    return (parts[-1], logit_scale * img_terms, grad_texts)


def solution(mesh):
    grid = Mesh(mesh.devices.reshape(4, 8, 2, 4), ("x", "z", "h", "dp"))
    rows = ("dp", "x", "z", "h")
    return jax.shard_map(
        step,
        mesh=grid,
        in_specs=(P(rows, None), P(rows, None), P(), P(None, rows)),
        out_specs=(P(None, rows), P(rows, None), P(rows, None)),
        check_vma=False,
    )
```

```python
import functools

import jax
import jax.numpy as jnp
from jax import lax
from jax.experimental import pallas as pl
from jax.experimental.pallas import tpu as pltpu
from jax.sharding import Mesh, PartitionSpec as P

VMEM = pl.BlockSpec(memory_space=pltpu.VMEM)
SMEM = pl.BlockSpec(memory_space=pltpu.SMEM)
PARAMS = pltpu.CompilerParams(vmem_limit_bytes=24 * 1024 * 1024)


def moved(value, axis, steps):
    count, lanes = lax.axis_size(axis), lax.axis_size("dp")
    pairs = [
        (i * lanes + c, (i + (steps if c % 2 == 0 else -steps)) % count * lanes + c)
        for i in range(count)
        for c in range(lanes)
    ]
    return lax.ppermute(value, (axis, "dp"), pairs)


def swapped(value, axis, bit):
    count = lax.axis_size(axis)
    return lax.ppermute(value, axis, [(i, i ^ bit) for i in range(count)])


def gather_z(block):
    half = lax.axis_size("z") // 2
    held = {0: block}
    for k in range(1, half):
        held[-k] = moved(held[1 - k], "z", 1)
        held[k] = moved(held[k - 1], "z", -1)
    held[half] = moved(held[half - 2], "z", -2)
    return held


def gather_xh(block):
    held = {(0, 0): block, (0, 1): moved(block, "h", 1)}
    for e in (0, 1):
        held[1, e] = moved(held[0, e], "x", -1)
        held[-1, e] = moved(held[0, e], "x", 1)
    held[2, 0] = moved(held[1, 0], "x", -1)
    held[2, 1] = moved(held[-1, 1], "x", 1)
    return held


def turn():
    return 1 - 2 * lax.rem(lax.axis_index("dp"), 2)


def image_id(offset):
    count = lax.axis_size("z")
    return lax.rem(lax.axis_index("z") + offset * turn() + count, count)


def text_id(offset, other):
    count = lax.axis_size("x")
    at_x = lax.rem(lax.axis_index("x") + offset * turn() + count, count)
    return 2 * at_x + lax.rem(lax.axis_index("h") + other, 2)


def low(value):
    return value.astype(jnp.bfloat16)


def wide(value):
    return value.astype(jnp.float32)


def across(column):
    return jnp.broadcast_to(column, (column.shape[0], 128)).T[0:1, :]


def down(row):
    return jnp.broadcast_to(row, (128, row.shape[1])).T


def product(left, right, left_dim, right_dim):
    return lax.dot_general(
        left, right, (((left_dim,), (right_dim,)), ((), ())), preferred_element_type=jnp.float32
    )


def stage_kernel(scale_ref, cot_in, img_in, txt_in, *refs):
    cot_ref, img_ref, txt_ref, gi_ref, gt_ref, match_ref, sems = refs
    copies = [
        pltpu.make_async_copy(source, target, sems.at[k])
        for k, (source, target) in enumerate(
            ((img_in, img_ref), (txt_in, txt_ref), (cot_in, cot_ref))
        )
    ]
    for copy in copies:
        copy.start()
    for copy in copies:
        copy.wait()
    img, txt = wide(img_ref[...]), wide(txt_ref[...])
    both = down(cot_ref[0:1, :] + cot_ref[1:2, :])[:, 0:1]
    gi_ref[...] = both * txt
    gt_ref[...] = both * img
    match_ref[...] = across(scale_ref[0] * jnp.sum(img * txt, axis=1, keepdims=True))


def scores_into(scale_ref, img_ref, txt_ref, s_ref):
    for c in range(0, txt_ref.shape[0], 256):
        part = product(img_ref[...], txt_ref[c : c + 256, :], 1, 1)
        s_ref[:, c : c + 256] = scale_ref[0] * part
    return jnp.max(s_ref[...], axis=0, keepdims=True)


def stats_into(s_ref, row_ref, col_top):
    col_sum = jnp.zeros_like(col_top)
    for b in range(row_ref.shape[0]):
        s = s_ref[128 * b : 128 * b + 128, :]
        top = jnp.max(s, axis=1, keepdims=True)
        total = jnp.sum(jnp.exp(s - top), axis=1, keepdims=True)
        row_ref[b : b + 1, :] = across(top + jnp.log(total))
        col_sum = col_sum + jnp.sum(jnp.exp(s - col_top), axis=0, keepdims=True)
    return col_sum


def pack(refs, into):
    for b, ref in enumerate(refs):
        into[128 * b : 128 * b + 128, :] = ref[...]


def stats_a_kernel(blocks, scale_ref, *refs):
    s_ref, row_ref, top_ref, sum_ref, img_ref, txt_ref = refs[-6:]
    pack(refs[:blocks], img_ref)
    pack(refs[blocks:-6], txt_ref)
    col_top = scores_into(scale_ref, img_ref, txt_ref, s_ref)
    top_ref[...] = col_top
    sum_ref[...] = stats_into(s_ref, row_ref, col_top)


def stats_b_kernel(offs, turns, late, scale_ref, cot_ref, *refs):
    row_a, txt_ref, top_ref, sum_ref, s_ref, row_ref, col_ref, img_ref, row_b = refs[late:]
    pack(refs[:late], img_ref)
    col_top = jnp.maximum(scores_into(scale_ref, img_ref, txt_ref, s_ref), top_ref[...])
    col_sum = stats_into(s_ref, row_b, col_top) + sum_ref[...] * jnp.exp(top_ref[...] - col_top)
    lse = col_top + jnp.log(col_sum)
    row_ref[...] = jnp.zeros_like(row_ref)
    col_ref[...] = jnp.zeros_like(col_ref)
    early = len(offs) - late
    for b, offset in enumerate(offs):
        part = row_a[b : b + 1, :] if b < early else row_b[b - early : b - early + 1, :]
        row_ref[pl.ds(image_id(offset), 1), :] = part
    for c, place in enumerate(turns):
        col_ref[pl.ds(text_id(*place), 1), :] = lse[:, 128 * c : 128 * c + 128]
    row_ref[pl.ds(len(offs) + image_id(0), 1), :] = cot_ref[0:1, :]
    col_ref[pl.ds(len(turns) + text_id(0, 0), 1), :] = cot_ref[1:2, :]


def weights_into(s_ref, w_ref, row_ref, col_ref, offs, turns):
    rows, cols = row_ref.shape[0] // 2, col_ref.shape[0] // 2
    places = [text_id(*place) for place in turns]
    col_lse = [col_ref[pl.ds(at, 1), :] for at in places]
    col_cot = [col_ref[pl.ds(cols + at, 1), :] for at in places]
    for b, offset in enumerate(offs):
        row_lse = down(row_ref[pl.ds(image_id(offset), 1), :])
        row_cot = down(row_ref[pl.ds(rows + image_id(offset), 1), :])
        for c in range(cols):
            s = s_ref[128 * b : 128 * b + 128, 128 * c : 128 * c + 128]
            w = row_cot * jnp.exp(s - row_lse) + col_cot[c] * jnp.exp(s - col_lse[c])
            w_ref[128 * b : 128 * b + 128, 128 * c : 128 * c + 128] = low(w)


def text_product(wa_ref, wb_ref, img_a, img_b, cols):
    return product(wa_ref[:, cols], img_a[...], 0, 0) + product(wb_ref[:, cols], img_b[...], 0, 0)


def weights_kernel(
    offs, turns, blocks, sa_ref, sb_ref, row_ref, col_ref, img_a, img_b, txt_ref, wa_ref, wb_ref, *out_refs
):
    weights_into(sb_ref, wb_ref, row_ref, col_ref, offs[-blocks:], turns)
    image_part = product(wb_ref[...], txt_ref[...], 1, 0)
    for k in range(blocks):
        out_refs[k][...] = low(image_part[128 * k : 128 * k + 128, :])
    weights_into(sa_ref, wa_ref, row_ref, col_ref, offs[:-blocks], turns)
    width = wa_ref.shape[1]
    text_part = text_product(wa_ref, wb_ref, img_a, img_b, slice(width - 256, width))
    for k in range(2):
        out_refs[blocks + k][...] = low(text_part[128 * k : 128 * k + 128, :])


def rest_kernel(rows, cols, wa_ref, wb_ref, img_a, img_b, txt_ref, gi_ref, gt_ref, *refs):
    match_ref, row_ref, col_ref = refs[:3]
    out_refs, loss_ref = refs[3:-1], refs[-1]
    image_part = product(wa_ref[...], txt_ref[...], 1, 0)
    out_refs[0][...] = image_part[:128, :] - gi_ref[...]
    for k in range(1, rows):
        out_refs[k][...] = image_part[128 * k : 128 * k + 128, :]
    text_part = text_product(wa_ref, wb_ref, img_a, img_b, slice(0, 128 * cols))
    out_refs[rows][...] = text_part[:128, :] - gt_ref[...]
    for k in range(1, cols):
        ref = out_refs[rows + k]
        ref[...] = text_part[128 * k : 128 * k + 128, :].astype(ref.dtype)
    loss_ref[0:1, :] = row_ref[pl.ds(image_id(0), 1), :] - match_ref[...]
    loss_ref[1:2, :] = col_ref[pl.ds(text_id(0, 0), 1), :] - match_ref[...]


def shape(*dims, dtype=jnp.float32):
    return jax.ShapeDtypeStruct(dims, dtype)


def call(kernel, specs, outs, flops, scratch=()):
    return pl.pallas_call(
        kernel,
        in_specs=specs,
        out_specs=[VMEM] * len(outs),
        out_shape=outs,
        scratch_shapes=scratch,
        compiler_params=PARAMS,
        cost_estimate=pl.CostEstimate(flops=flops, bytes_accessed=4 << 20, transcendentals=1 << 20),
    )


def merge_lse(first, second):
    top = jnp.maximum(first, second)
    return top + jnp.log(jnp.exp(first - top) + jnp.exp(second - top))


def step(images, texts, scale, cotangent):
    n, width = images.shape
    logit_scale = scale[0]
    z_n, x_n = lax.axis_size("z"), lax.axis_size("x")
    c_n = 2 * x_n
    half = z_n // 2
    offs = [0] + [s * k for k in range(1, half) for s in (1, -1)] + [half]
    turns = [(d, e) for d in (0, 1, -1, 2) for e in (0, 1)]
    cols = c_n * n
    early = half + 1
    late = z_n - early
    tile = 2 * cols * width * n
    sent = shape(n, width, dtype=jnp.bfloat16)
    kept = shape(n, width)
    img_held = gather_z(images)
    txt_held = gather_xh(texts)
    cot, img_own, txt_own, base_i, base_t, matched = call(
        stage_kernel,
        [SMEM] + [pl.BlockSpec(memory_space=pltpu.HBM)] * 3,
        [shape(2, n), sent, sent, kept, kept, shape(1, n)],
        tile // 8,
        [pltpu.SemaphoreType.DMA((3,))],
    )(scale, *[pltpu.with_memory_space_constraint(v, pltpu.HBM) for v in (cotangent, images, texts)])
    img_held[0], txt_held[0, 0] = img_own, txt_own
    s_a, row_a, top_a, sum_a, img_a, txt = call(
        functools.partial(stats_a_kernel, early),
        [SMEM] + [VMEM] * (early + c_n),
        [shape(early * n, cols), shape(early, n), shape(1, cols), shape(1, cols)]
        + [shape(r, width, dtype=jnp.bfloat16) for r in (early * n, cols)],
        early * tile,
    )(scale, *[img_held[o] for o in offs[:early]], *[txt_held[t] for t in turns])
    s_b, row_msg, col_msg, img_b = call(
        functools.partial(stats_b_kernel, offs, turns, late),
        [SMEM] + [VMEM] * (late + 5),
        [shape(late * n, cols), shape(2 * z_n, n), shape(2 * c_n, n)]
        + [shape(late * n, width, dtype=jnp.bfloat16)],
        late * tile,
        [pltpu.VMEM((late, n), jnp.float32)],
    )(scale, cot, *[img_held[o] for o in offs[early:]], row_a, txt, top_a, sum_a)

    def merged(mine, got):
        sums = lax.broadcasted_iota(jnp.int32, mine.shape, 0) >= mine.shape[0] // 2
        return jnp.where(sums, mine + got, merge_lse(mine, got))

    for z_bit, col_axis, col_bit in ((7, "h", 1), (2, "x", 3), (1, "x", 1)):
        row_got = swapped(row_msg, "z", z_bit)
        col_got = swapped(col_msg, col_axis, col_bit)
        row_msg = merged(row_msg, row_got)
        col_msg = merged(col_msg, col_got)

    w_a, w_b, up, down_msg, far, fore, back = call(
        functools.partial(weights_kernel, offs, turns, late),
        [VMEM] * 7,
        [shape(r * n, cols, dtype=jnp.bfloat16) for r in (early, late)] + [sent] * (late + 2),
        4 * tile,
    )(s_a, s_b, row_msg, col_msg, img_a, img_b, txt)
    direct = ((1, 1), (-1, 0))
    parts = call(
        functools.partial(rest_kernel, early, c_n - 2),
        [VMEM] * 10,
        [kept] * early
        + [sent if t in direct else kept for t in turns[:-2]]
        + [shape(2, n)],
        12 * tile,
    )(w_a, w_b, img_a, img_b, txt, base_i, base_t, matched, row_msg, col_msg)
    part = dict(zip(offs[:early], parts[:early]))
    piece = dict(zip(turns[:-2], parts[early:-1]))

    far = wide(moved(far, "z", 2))
    up = moved(up, "z", 1)
    down_msg = moved(down_msg, "z", -1)
    for k in range(half - 2, 0, -1):
        total = part[k] + wide(up)
        if k == half - 2:
            total = total + far
        up = moved(low(total), "z", 1)
        down_msg = moved(low(part[-k] + wide(down_msg)), "z", -1)
    img_terms = part[0] + wide(up) + wide(down_msg)

    fore = moved(fore, "x", 1)
    back = moved(back, "x", -1)
    fore1 = moved(piece[1, 1], "x", 1)
    back0 = moved(piece[-1, 0], "x", -1)
    fore0 = moved(low(piece[1, 0] + wide(fore)), "x", 1)
    back1 = moved(low(piece[-1, 1] + wide(back)), "x", -1)
    other = moved(low(piece[0, 1] + wide(fore1) + wide(back1)), "h", 1)

    grad_texts = logit_scale * (piece[0, 0] + wide(fore0) + wide(back0) + wide(other))
    return (parts[-1], logit_scale * img_terms, grad_texts)


def solution(mesh):
    grid = Mesh(mesh.devices.reshape(4, 8, 2, 4), ("x", "z", "h", "dp"))
    rows = ("dp", "x", "z", "h")
    return jax.shard_map(
        step,
        mesh=grid,
        in_specs=(P(rows, None), P(rows, None), P(), P(None, rows)),
        out_specs=(P(None, rows), P(rows, None), P(rows, None)),
        check_vma=False,
    )
```

```python
import functools

import jax
import jax.numpy as jnp
from jax import lax
from jax.experimental import pallas as pl
from jax.experimental.pallas import tpu as pltpu
from jax.sharding import Mesh, PartitionSpec as P

VMEM = pl.BlockSpec(memory_space=pltpu.VMEM)
SMEM = pl.BlockSpec(memory_space=pltpu.SMEM)
PARAMS = pltpu.CompilerParams(vmem_limit_bytes=24 * 1024 * 1024)


def moved(value, axis, steps):
    count, lanes = lax.axis_size(axis), lax.axis_size("dp")
    pairs = [
        (i * lanes + c, (i + (steps if c % 2 == 0 else -steps)) % count * lanes + c)
        for i in range(count)
        for c in range(lanes)
    ]
    return lax.ppermute(value, (axis, "dp"), pairs)


def swapped(value, axis, bit):
    count = lax.axis_size(axis)
    return lax.ppermute(value, axis, [(i, i ^ bit) for i in range(count)])


def gather_z(block):
    half = lax.axis_size("z") // 2
    held = {0: block}
    for k in range(1, half):
        held[-k] = moved(held[1 - k], "z", 1)
        held[k] = moved(held[k - 1], "z", -1)
    held[half] = moved(held[half - 2], "z", -2)
    return held


def gather_xh(block):
    held = {(0, 0): block, (0, 1): moved(block, "h", 1)}
    for e in (0, 1):
        held[1, e] = moved(held[0, e], "x", -1)
        held[-1, e] = moved(held[0, e], "x", 1)
    held[2, 0] = moved(held[1, 0], "x", -1)
    held[2, 1] = moved(held[-1, 1], "x", 1)
    return held


def turn():
    return 1 - 2 * lax.rem(lax.axis_index("dp"), 2)


def image_id(offset):
    count = lax.axis_size("z")
    return lax.rem(lax.axis_index("z") + offset * turn() + count, count)


def text_id(offset, other):
    count = lax.axis_size("x")
    at_x = lax.rem(lax.axis_index("x") + offset * turn() + count, count)
    return 2 * at_x + lax.rem(lax.axis_index("h") + other, 2)


def low(value):
    return value.astype(jnp.bfloat16)


def wide(value):
    return value.astype(jnp.float32)


def across(column):
    return jnp.broadcast_to(column, (column.shape[0], 128)).T[0:1, :]


def down(row):
    return jnp.broadcast_to(row, (128, row.shape[1])).T


def product(left, right, left_dim, right_dim):
    return lax.dot_general(
        left, right, (((left_dim,), (right_dim,)), ((), ())), preferred_element_type=jnp.float32
    )


def stage_kernel(scale_ref, cot_in, img_in, txt_in, *refs):
    cot_ref, img_ref, txt_ref, gi_ref, gt_ref, match_ref, sems = refs
    copies = [
        pltpu.make_async_copy(source, target, sems.at[k])
        for k, (source, target) in enumerate(
            ((img_in, img_ref), (txt_in, txt_ref), (cot_in, cot_ref))
        )
    ]
    for copy in copies:
        copy.start()
    for copy in copies:
        copy.wait()
    img, txt = wide(img_ref[...]), wide(txt_ref[...])
    both = down(cot_ref[0:1, :] + cot_ref[1:2, :])[:, 0:1]
    gi_ref[...] = both * txt
    gt_ref[...] = both * img
    match_ref[...] = across(scale_ref[0] * jnp.sum(img * txt, axis=1, keepdims=True))


def scores_into(scale_ref, img_ref, txt_ref, s_ref):
    for c in range(0, txt_ref.shape[0], 256):
        part = product(img_ref[...], txt_ref[c : c + 256, :], 1, 1)
        s_ref[:, c : c + 256] = scale_ref[0] * part
    return jnp.max(s_ref[...], axis=0, keepdims=True)


def stats_into(s_ref, row_ref, col_top):
    col_sum = jnp.zeros_like(col_top)
    for b in range(row_ref.shape[0]):
        s = s_ref[128 * b : 128 * b + 128, :]
        top = jnp.max(s, axis=1, keepdims=True)
        total = jnp.sum(jnp.exp(s - top), axis=1, keepdims=True)
        row_ref[b : b + 1, :] = across(top + jnp.log(total))
        col_sum = col_sum + jnp.sum(jnp.exp(s - col_top), axis=0, keepdims=True)
    return col_sum


def pack(refs, into):
    for b, ref in enumerate(refs):
        into[128 * b : 128 * b + 128, :] = ref[...]


def stats_a_kernel(blocks, scale_ref, *refs):
    s_ref, row_ref, top_ref, sum_ref, img_ref, txt_ref = refs[-6:]
    pack(refs[:blocks], img_ref)
    pack(refs[blocks:-6], txt_ref)
    col_top = scores_into(scale_ref, img_ref, txt_ref, s_ref)
    top_ref[...] = col_top
    sum_ref[...] = stats_into(s_ref, row_ref, col_top)


def stats_b_kernel(offs, turns, late, scale_ref, cot_ref, *refs):
    row_a, txt_ref, top_ref, sum_ref, s_ref, row_ref, col_ref, img_ref, row_b = refs[late:]
    pack(refs[:late], img_ref)
    col_top = jnp.maximum(scores_into(scale_ref, img_ref, txt_ref, s_ref), top_ref[...])
    col_sum = stats_into(s_ref, row_b, col_top) + sum_ref[...] * jnp.exp(top_ref[...] - col_top)
    lse = col_top + jnp.log(col_sum)
    row_ref[...] = jnp.zeros_like(row_ref)
    col_ref[...] = jnp.zeros_like(col_ref)
    early = len(offs) - late
    for b, offset in enumerate(offs):
        part = row_a[b : b + 1, :] if b < early else row_b[b - early : b - early + 1, :]
        row_ref[pl.ds(image_id(offset), 1), :] = part
    for c, place in enumerate(turns):
        col_ref[pl.ds(text_id(*place), 1), :] = lse[:, 128 * c : 128 * c + 128]
    row_ref[pl.ds(len(offs) + image_id(0), 1), :] = cot_ref[0:1, :]
    col_ref[pl.ds(len(turns) + text_id(0, 0), 1), :] = cot_ref[1:2, :]


def weights_into(s_ref, w_ref, row_ref, col_ref, offs, turns):
    rows, cols = row_ref.shape[0] // 2, col_ref.shape[0] // 2
    places = [text_id(*place) for place in turns]
    col_lse = [col_ref[pl.ds(at, 1), :] for at in places]
    col_cot = [col_ref[pl.ds(cols + at, 1), :] for at in places]
    for b, offset in enumerate(offs):
        row_lse = down(row_ref[pl.ds(image_id(offset), 1), :])
        row_cot = down(row_ref[pl.ds(rows + image_id(offset), 1), :])
        for c in range(cols):
            s = s_ref[128 * b : 128 * b + 128, 128 * c : 128 * c + 128]
            w = row_cot * jnp.exp(s - row_lse) + col_cot[c] * jnp.exp(s - col_lse[c])
            w_ref[128 * b : 128 * b + 128, 128 * c : 128 * c + 128] = low(w)


def text_product(wa_ref, wb_ref, img_a, img_b, cols):
    return product(wa_ref[:, cols], img_a[...], 0, 0) + product(wb_ref[:, cols], img_b[...], 0, 0)


def weights_kernel(
    offs, turns, blocks, sa_ref, sb_ref, row_ref, col_ref, img_a, img_b, txt_ref, wa_ref, wb_ref, *out_refs
):
    weights_into(sb_ref, wb_ref, row_ref, col_ref, offs[-blocks:], turns)
    image_part = product(wb_ref[...], txt_ref[...], 1, 0)
    for k in range(blocks):
        out_refs[k][...] = low(image_part[128 * k : 128 * k + 128, :])
    weights_into(sa_ref, wa_ref, row_ref, col_ref, offs[:-blocks], turns)
    width = wa_ref.shape[1]
    text_part = text_product(wa_ref, wb_ref, img_a, img_b, slice(width - 256, width))
    for k in range(2):
        out_refs[blocks + k][...] = low(text_part[128 * k : 128 * k + 128, :])


def rest_kernel(rows, cols, wa_ref, wb_ref, img_a, img_b, txt_ref, gi_ref, gt_ref, *refs):
    match_ref, row_ref, col_ref = refs[:3]
    out_refs, loss_ref = refs[3:-1], refs[-1]
    image_part = product(wa_ref[...], txt_ref[...], 1, 0)
    out_refs[0][...] = image_part[:128, :] - gi_ref[...]
    for k in range(1, rows):
        out_refs[k][...] = image_part[128 * k : 128 * k + 128, :]
    text_part = text_product(wa_ref, wb_ref, img_a, img_b, slice(0, 128 * cols))
    out_refs[rows][...] = text_part[:128, :] - gt_ref[...]
    for k in range(1, cols):
        ref = out_refs[rows + k]
        ref[...] = text_part[128 * k : 128 * k + 128, :].astype(ref.dtype)
    loss_ref[0:1, :] = row_ref[pl.ds(image_id(0), 1), :] - match_ref[...]
    loss_ref[1:2, :] = col_ref[pl.ds(text_id(0, 0), 1), :] - match_ref[...]


def shape(*dims, dtype=jnp.float32):
    return jax.ShapeDtypeStruct(dims, dtype)


def call(kernel, specs, outs, flops, scratch=()):
    return pl.pallas_call(
        kernel,
        in_specs=specs,
        out_specs=[VMEM] * len(outs),
        out_shape=outs,
        scratch_shapes=scratch,
        compiler_params=PARAMS,
        cost_estimate=pl.CostEstimate(flops=flops, bytes_accessed=4 << 20, transcendentals=1 << 20),
    )


def merge_lse(first, second):
    top = jnp.maximum(first, second)
    return top + jnp.log(jnp.exp(first - top) + jnp.exp(second - top))


def step(images, texts, scale, cotangent):
    n, width = images.shape
    logit_scale = scale[0]
    z_n, x_n = lax.axis_size("z"), lax.axis_size("x")
    c_n = 2 * x_n
    half = z_n // 2
    offs = [0] + [s * k for k in range(1, half) for s in (1, -1)] + [half]
    turns = [(d, e) for d in (0, 1, -1, 2) for e in (0, 1)]
    cols = c_n * n
    early = half + 1
    late = z_n - early
    tile = 2 * cols * width * n
    sent = shape(n, width, dtype=jnp.bfloat16)
    kept = shape(n, width)
    img_held = gather_z(images)
    txt_held = gather_xh(texts)
    cot, img_own, txt_own, base_i, base_t, matched = call(
        stage_kernel,
        [SMEM] + [pl.BlockSpec(memory_space=pltpu.HBM)] * 3,
        [shape(2, n), sent, sent, kept, kept, shape(1, n)],
        tile // 8,
        [pltpu.SemaphoreType.DMA((3,))],
    )(scale, *[pltpu.with_memory_space_constraint(v, pltpu.HBM) for v in (cotangent, images, texts)])
    img_held[0], txt_held[0, 0] = img_own, txt_own
    s_a, row_a, top_a, sum_a, img_a, txt = call(
        functools.partial(stats_a_kernel, early),
        [SMEM] + [VMEM] * (early + c_n),
        [shape(early * n, cols), shape(early, n), shape(1, cols), shape(1, cols)]
        + [shape(r, width, dtype=jnp.bfloat16) for r in (early * n, cols)],
        early * tile,
    )(scale, *[img_held[o] for o in offs[:early]], *[txt_held[t] for t in turns])
    s_b, row_msg, col_msg, img_b = call(
        functools.partial(stats_b_kernel, offs, turns, late),
        [SMEM] + [VMEM] * (late + 5),
        [shape(late * n, cols), shape(2 * z_n, n), shape(2 * c_n, n)]
        + [shape(late * n, width, dtype=jnp.bfloat16)],
        late * tile,
        [pltpu.VMEM((late, n), jnp.float32)],
    )(scale, cot, *[img_held[o] for o in offs[early:]], row_a, txt, top_a, sum_a)

    def merged(mine, got, sums):
        return jnp.where(sums, mine + got, merge_lse(mine, got))

    row_sums = lax.broadcasted_iota(jnp.int32, row_msg.shape, 0) >= z_n
    col_sums = lax.broadcasted_iota(jnp.float32, col_msg.shape, 0) > c_n - 0.5
    for z_bit, col_axis, col_bit in ((7, "h", 1), (2, "x", 3), (1, "x", 1)):
        row_got = swapped(row_msg, "z", z_bit)
        col_got = swapped(col_msg, col_axis, col_bit)
        row_msg = merged(row_msg, row_got, row_sums)
        col_msg = merged(col_msg, col_got, col_sums)

    w_a, w_b, up, down_msg, far, fore, back = call(
        functools.partial(weights_kernel, offs, turns, late),
        [VMEM] * 7,
        [shape(r * n, cols, dtype=jnp.bfloat16) for r in (early, late)] + [sent] * (late + 2),
        4 * tile,
    )(s_a, s_b, row_msg, col_msg, img_a, img_b, txt)
    direct = ((1, 1), (-1, 0))
    parts = call(
        functools.partial(rest_kernel, early, c_n - 2),
        [VMEM] * 10,
        [kept] * early
        + [sent if t in direct else kept for t in turns[:-2]]
        + [shape(2, n)],
        12 * tile,
    )(w_a, w_b, img_a, img_b, txt, base_i, base_t, matched, row_msg, col_msg)
    part = dict(zip(offs[:early], parts[:early]))
    piece = dict(zip(turns[:-2], parts[early:-1]))

    far = wide(moved(far, "z", 2))
    up = moved(up, "z", 1)
    down_msg = moved(down_msg, "z", -1)
    for k in range(half - 2, 0, -1):
        total = part[k] + wide(up)
        if k == half - 2:
            total = total + far
        up = moved(low(total), "z", 1)
        down_msg = moved(low(part[-k] + wide(down_msg)), "z", -1)
    img_terms = part[0] + wide(up) + wide(down_msg)

    fore = moved(fore, "x", 1)
    back = moved(back, "x", -1)
    fore1 = moved(piece[1, 1], "x", 1)
    back0 = moved(piece[-1, 0], "x", -1)
    fore0 = moved(low(piece[1, 0] + wide(fore)), "x", 1)
    back1 = moved(low(piece[-1, 1] + wide(back)), "x", -1)
    other = moved(low(piece[0, 1] + wide(fore1) + wide(back1)), "h", 1)

    grad_texts = logit_scale * (piece[0, 0] + wide(fore0) + wide(back0) + wide(other))
    return (parts[-1], logit_scale * img_terms, grad_texts)


def solution(mesh):
    grid = Mesh(mesh.devices.reshape(4, 8, 2, 4), ("x", "z", "h", "dp"))
    rows = ("dp", "x", "z", "h")
    return jax.shard_map(
        step,
        mesh=grid,
        in_specs=(P(rows, None), P(rows, None), P(), P(None, rows)),
        out_specs=(P(None, rows), P(rows, None), P(rows, None)),
        check_vma=False,
    )
```

```python
import functools

import jax
import jax.numpy as jnp
from jax import lax
from jax.experimental import pallas as pl
from jax.experimental.pallas import tpu as pltpu
from jax.sharding import Mesh, PartitionSpec as P

VMEM = pl.BlockSpec(memory_space=pltpu.VMEM)
SMEM = pl.BlockSpec(memory_space=pltpu.SMEM)
PARAMS = pltpu.CompilerParams(vmem_limit_bytes=24 * 1024 * 1024)


def moved(value, axis, steps):
    count, lanes = lax.axis_size(axis), lax.axis_size("dp")
    pairs = [
        (i * lanes + c, (i + (steps if c % 2 == 0 else -steps)) % count * lanes + c)
        for i in range(count)
        for c in range(lanes)
    ]
    return lax.ppermute(value, (axis, "dp"), pairs)


def swapped(value, axis, bit):
    count = lax.axis_size(axis)
    return lax.ppermute(value, axis, [(i, i ^ bit) for i in range(count)])


def gather_z(block):
    half = lax.axis_size("z") // 2
    held = {0: block}
    for k in range(1, half):
        held[-k] = moved(held[1 - k], "z", 1)
        held[k] = moved(held[k - 1], "z", -1)
    held[half] = moved(held[half - 2], "z", -2)
    return held


def gather_xh(block):
    held = {(0, 0): block, (0, 1): moved(block, "h", 1)}
    for e in (0, 1):
        held[1, e] = moved(held[0, e], "x", -1)
        held[-1, e] = moved(held[0, e], "x", 1)
    held[2, 0] = moved(held[1, 0], "x", -1)
    held[2, 1] = moved(held[-1, 1], "x", 1)
    return held


def turn():
    return 1 - 2 * lax.rem(lax.axis_index("dp"), 2)


def image_id(offset):
    count = lax.axis_size("z")
    return lax.rem(lax.axis_index("z") + offset * turn() + count, count)


def text_id(offset, other):
    count = lax.axis_size("x")
    at_x = lax.rem(lax.axis_index("x") + offset * turn() + count, count)
    return 2 * at_x + lax.rem(lax.axis_index("h") + other, 2)


def low(value):
    return value.astype(jnp.bfloat16)


def wide(value):
    return value.astype(jnp.float32)


def across(column):
    return jnp.broadcast_to(column, (column.shape[0], 128)).T[0:1, :]


def down(row):
    return jnp.broadcast_to(row, (128, row.shape[1])).T


def product(left, right, left_dim, right_dim):
    return lax.dot_general(
        left, right, (((left_dim,), (right_dim,)), ((), ())), preferred_element_type=jnp.float32
    )


def stage_kernel(scale_ref, cot_in, img_in, txt_in, *refs):
    cot_ref, img_ref, txt_ref, gi_ref, gt_ref, match_ref, sems = refs
    copies = [
        pltpu.make_async_copy(source, target, sems.at[k])
        for k, (source, target) in enumerate(
            ((img_in, img_ref), (txt_in, txt_ref), (cot_in, cot_ref))
        )
    ]
    for copy in copies:
        copy.start()
    for copy in copies:
        copy.wait()
    img, txt = wide(img_ref[...]), wide(txt_ref[...])
    both = down(cot_ref[0:1, :] + cot_ref[1:2, :])[:, 0:1]
    gi_ref[...] = both * txt
    gt_ref[...] = both * img
    match_ref[...] = across(scale_ref[0] * jnp.sum(img * txt, axis=1, keepdims=True))


def scores_into(scale_ref, img_ref, txt_ref, s_ref):
    for c in range(0, txt_ref.shape[0], 256):
        part = product(img_ref[...], txt_ref[c : c + 256, :], 1, 1)
        s_ref[:, c : c + 256] = scale_ref[0] * part
    return jnp.max(s_ref[...], axis=0, keepdims=True)


def stats_into(s_ref, row_ref, col_top):
    col_sum = jnp.zeros_like(col_top)
    for b in range(row_ref.shape[0]):
        s = s_ref[128 * b : 128 * b + 128, :]
        top = jnp.max(s, axis=1, keepdims=True)
        total = jnp.sum(jnp.exp(s - top), axis=1, keepdims=True)
        row_ref[b : b + 1, :] = across(top + jnp.log(total))
        col_sum = col_sum + jnp.sum(jnp.exp(s - col_top), axis=0, keepdims=True)
    return col_sum


def pack(refs, into):
    for b, ref in enumerate(refs):
        into[128 * b : 128 * b + 128, :] = ref[...]


def stats_a_kernel(blocks, scale_ref, *refs):
    s_ref, row_ref, top_ref, sum_ref, img_ref, txt_ref = refs[-6:]
    pack(refs[:blocks], img_ref)
    pack(refs[blocks:-6], txt_ref)
    col_top = scores_into(scale_ref, img_ref.at[: 128 * blocks, :], txt_ref, s_ref)
    top_ref[...] = col_top
    sum_ref[...] = stats_into(s_ref, row_ref, col_top)


def stats_b_kernel(offs, turns, late, scale_ref, cot_ref, *refs):
    row_a, txt_ref, top_ref, sum_ref, _, s_ref, row_ref, col_ref, img_all, row_b = refs[late:]
    img_ref = img_all.at[128 * (len(offs) - late) :, :]
    pack(refs[:late], img_ref)
    col_top = jnp.maximum(scores_into(scale_ref, img_ref, txt_ref, s_ref), top_ref[...])
    col_sum = stats_into(s_ref, row_b, col_top) + sum_ref[...] * jnp.exp(top_ref[...] - col_top)
    lse = col_top + jnp.log(col_sum)
    row_ref[...] = jnp.zeros_like(row_ref)
    col_ref[...] = jnp.zeros_like(col_ref)
    early = len(offs) - late
    for b, offset in enumerate(offs):
        part = row_a[b : b + 1, :] if b < early else row_b[b - early : b - early + 1, :]
        row_ref[pl.ds(image_id(offset), 1), :] = part
    for c, place in enumerate(turns):
        col_ref[pl.ds(text_id(*place), 1), :] = lse[:, 128 * c : 128 * c + 128]
    row_ref[pl.ds(len(offs) + image_id(0), 1), :] = cot_ref[0:1, :]
    col_ref[pl.ds(len(turns) + text_id(0, 0), 1), :] = cot_ref[1:2, :]


def weights_into(s_ref, w_ref, row_ref, col_ref, offs, turns):
    rows, cols = row_ref.shape[0] // 2, col_ref.shape[0] // 2
    places = [text_id(*place) for place in turns]
    col_lse = [col_ref[pl.ds(at, 1), :] for at in places]
    col_cot = [col_ref[pl.ds(cols + at, 1), :] for at in places]
    for b, offset in enumerate(offs):
        row_lse = down(row_ref[pl.ds(image_id(offset), 1), :])
        row_cot = down(row_ref[pl.ds(rows + image_id(offset), 1), :])
        for c in range(cols):
            s = s_ref[128 * b : 128 * b + 128, 128 * c : 128 * c + 128]
            w = row_cot * jnp.exp(s - row_lse) + col_cot[c] * jnp.exp(s - col_lse[c])
            w_ref[128 * b : 128 * b + 128, 128 * c : 128 * c + 128] = low(w)


def first_kernel(offs, turns, s_ref, row_ref, col_ref, txt_ref, w_all, *out_refs):
    w_ref = w_all.at[w_all.shape[0] - s_ref.shape[0] :, :]
    weights_into(s_ref, w_ref, row_ref, col_ref, offs[-len(out_refs) :], turns)
    image_part = product(w_ref[...], txt_ref[...], 1, 0)
    for k, ref in enumerate(out_refs):
        ref[...] = low(image_part[128 * k : 128 * k + 128, :])


def second_kernel(offs, turns, s_ref, row_ref, col_ref, img_ref, _, w_ref, *out_refs):
    rows, width = s_ref.shape
    weights_into(s_ref, w_ref.at[:rows, :], row_ref, col_ref, offs[: rows // 128], turns)
    text_part = product(w_ref[:, width - 256 :], img_ref[...], 0, 0)
    for k, ref in enumerate(out_refs):
        ref[...] = low(text_part[128 * k : 128 * k + 128, :])


def rest_kernel(rows, cols, w_ref, img_ref, txt_ref, gi_ref, gt_ref, *refs):
    match_ref, row_ref, col_ref = refs[:3]
    out_refs, loss_ref = refs[3:-1], refs[-1]
    image_part = product(w_ref[: 128 * rows, :], txt_ref[...], 1, 0)
    out_refs[0][...] = image_part[:128, :] - gi_ref[...]
    for k in range(1, rows):
        out_refs[k][...] = image_part[128 * k : 128 * k + 128, :]
    text_part = product(w_ref[:, : 128 * cols], img_ref[...], 0, 0)
    out_refs[rows][...] = text_part[:128, :] - gt_ref[...]
    for k in range(1, cols):
        ref = out_refs[rows + k]
        ref[...] = text_part[128 * k : 128 * k + 128, :].astype(ref.dtype)
    loss_ref[0:1, :] = row_ref[pl.ds(image_id(0), 1), :] - match_ref[...]
    loss_ref[1:2, :] = col_ref[pl.ds(text_id(0, 0), 1), :] - match_ref[...]


def shape(*dims, dtype=jnp.float32):
    return jax.ShapeDtypeStruct(dims, dtype)


def call(kernel, specs, outs, flops, scratch=(), aliases=None):
    return pl.pallas_call(
        kernel,
        in_specs=specs,
        out_specs=[VMEM] * len(outs),
        out_shape=outs,
        scratch_shapes=scratch,
        input_output_aliases=aliases or {},
        compiler_params=PARAMS,
        cost_estimate=pl.CostEstimate(flops=flops, bytes_accessed=4 << 20, transcendentals=1 << 20),
    )


def merge_lse(first, second):
    top = jnp.maximum(first, second)
    return top + jnp.log(jnp.exp(first - top) + jnp.exp(second - top))


def step(images, texts, scale, cotangent):
    n, width = images.shape
    logit_scale = scale[0]
    z_n, x_n = lax.axis_size("z"), lax.axis_size("x")
    c_n = 2 * x_n
    half = z_n // 2
    offs = [0] + [s * k for k in range(1, half) for s in (1, -1)] + [half]
    turns = [(d, e) for d in (0, 1, -1, 2) for e in (0, 1)]
    rows, cols = z_n * n, c_n * n
    early = half + 1
    late = z_n - early
    tile = 2 * cols * width * n
    sent = shape(n, width, dtype=jnp.bfloat16)
    kept = shape(n, width)
    img_held = gather_z(images)
    txt_held = gather_xh(texts)
    cot, img_own, txt_own, base_i, base_t, matched = call(
        stage_kernel,
        [SMEM] + [pl.BlockSpec(memory_space=pltpu.HBM)] * 3,
        [shape(2, n), sent, sent, kept, kept, shape(1, n)],
        tile // 8,
        [pltpu.SemaphoreType.DMA((3,))],
    )(scale, *[pltpu.with_memory_space_constraint(v, pltpu.HBM) for v in (cotangent, images, texts)])
    img_held[0], txt_held[0, 0] = img_own, txt_own
    s_a, row_a, top_a, sum_a, img_a, txt = call(
        functools.partial(stats_a_kernel, early),
        [SMEM] + [VMEM] * (early + c_n),
        [shape(early * n, cols), shape(early, n), shape(1, cols), shape(1, cols)]
        + [shape(r, width, dtype=jnp.bfloat16) for r in (rows, cols)],
        early * tile,
    )(scale, *[img_held[o] for o in offs[:early]], *[txt_held[t] for t in turns])
    s_b, row_msg, col_msg, img = call(
        functools.partial(stats_b_kernel, offs, turns, late),
        [SMEM] + [VMEM] * (late + 6),
        [shape(late * n, cols), shape(2 * z_n, n), shape(2 * c_n, n)]
        + [shape(rows, width, dtype=jnp.bfloat16)],
        late * tile,
        [pltpu.VMEM((late, n), jnp.float32)],
        {late + 6: 3},
    )(scale, cot, *[img_held[o] for o in offs[early:]], row_a, txt, top_a, sum_a, img_a)

    def merged(mine, got, sums):
        return jnp.where(sums, mine + got, merge_lse(mine, got))

    row_sums = lax.broadcasted_iota(jnp.int32, row_msg.shape, 0) >= z_n
    col_sums = lax.broadcasted_iota(jnp.float32, col_msg.shape, 0) > c_n - 0.5
    for z_bit, col_axis, col_bit in ((7, "h", 1), (2, "x", 3), (1, "x", 1)):
        row_got = swapped(row_msg, "z", z_bit)
        col_got = swapped(col_msg, col_axis, col_bit)
        row_msg = merged(row_msg, row_got, row_sums)
        col_msg = merged(col_msg, col_got, col_sums)

    whole = shape(rows, cols, dtype=jnp.bfloat16)
    w_late, up, down_msg, far = call(
        functools.partial(first_kernel, offs, turns), [VMEM] * 4, [whole] + [sent] * late, 3 * tile
    )(s_b, row_msg, col_msg, txt)
    weights, fore, back = call(
        functools.partial(second_kernel, offs, turns),
        [VMEM] * 5,
        [whole] + [sent] * 2,
        3 * tile,
        (),
        {4: 0},
    )(s_a, row_msg, col_msg, img, w_late)
    direct = ((1, 1), (-1, 0))
    parts = call(
        functools.partial(rest_kernel, early, c_n - 2),
        [VMEM] * 8,
        [kept] * early
        + [sent if t in direct else kept for t in turns[:-2]]
        + [shape(2, n)],
        12 * tile,
    )(weights, img, txt, base_i, base_t, matched, row_msg, col_msg)
    part = dict(zip(offs[:early], parts[:early]))
    piece = dict(zip(turns[:-2], parts[early:-1]))

    far = wide(moved(far, "z", 2))
    up = moved(up, "z", 1)
    down_msg = moved(down_msg, "z", -1)
    for k in range(half - 2, 0, -1):
        total = part[k] + wide(up)
        if k == half - 2:
            total = total + far
        up = moved(low(total), "z", 1)
        down_msg = moved(low(part[-k] + wide(down_msg)), "z", -1)
    img_terms = part[0] + wide(up) + wide(down_msg)

    fore = moved(fore, "x", 1)
    back = moved(back, "x", -1)
    fore1 = moved(piece[1, 1], "x", 1)
    back0 = moved(piece[-1, 0], "x", -1)
    fore0 = moved(low(piece[1, 0] + wide(fore)), "x", 1)
    back1 = moved(low(piece[-1, 1] + wide(back)), "x", -1)
    other = moved(low(piece[0, 1] + wide(fore1) + wide(back1)), "h", 1)

    grad_texts = logit_scale * (piece[0, 0] + wide(fore0) + wide(back0) + wide(other))
    return (parts[-1], logit_scale * img_terms, grad_texts)


def solution(mesh):
    grid = Mesh(mesh.devices.reshape(4, 8, 2, 4), ("x", "z", "h", "dp"))
    rows = ("dp", "x", "z", "h")
    return jax.shard_map(
        step,
        mesh=grid,
        in_specs=(P(rows, None), P(rows, None), P(), P(None, rows)),
        out_specs=(P(None, rows), P(rows, None), P(rows, None)),
        check_vma=False,
    )
```

```python
import functools

import jax
import jax.numpy as jnp
from jax import lax
from jax.experimental import pallas as pl
from jax.experimental.pallas import tpu as pltpu
from jax.sharding import Mesh, PartitionSpec as P

VMEM = pl.BlockSpec(memory_space=pltpu.VMEM)
SMEM = pl.BlockSpec(memory_space=pltpu.SMEM)
PARAMS = pltpu.CompilerParams(vmem_limit_bytes=24 * 1024 * 1024)


def moved(value, axis, steps):
    count, lanes = lax.axis_size(axis), lax.axis_size("dp")
    pairs = [
        (i * lanes + c, (i + (steps if c % 2 == 0 else -steps)) % count * lanes + c)
        for i in range(count)
        for c in range(lanes)
    ]
    return lax.ppermute(value, (axis, "dp"), pairs)


def swapped(value, axis, bit):
    count = lax.axis_size(axis)
    return lax.ppermute(value, axis, [(i, i ^ bit) for i in range(count)])


def gather_z(block):
    half = lax.axis_size("z") // 2
    held = {0: block}
    for k in range(1, half):
        held[-k] = moved(held[1 - k], "z", 1)
        held[k] = moved(held[k - 1], "z", -1)
    held[half] = moved(held[1], "z", 1 - half)
    return held


def gather_xh(block):
    held = {(0, 0): block, (0, 1): moved(block, "h", 1)}
    for e in (0, 1):
        held[1, e] = moved(held[0, e], "x", -1)
        held[-1, e] = moved(held[0, e], "x", 1)
    held[2, 0] = moved(held[1, 0], "x", -1)
    held[2, 1] = moved(held[-1, 1], "x", 1)
    return held


def turn():
    return 1 - 2 * lax.rem(lax.axis_index("dp"), 2)


def image_id(offset):
    count = lax.axis_size("z")
    return lax.rem(lax.axis_index("z") + offset * turn() + count, count)


def text_id(offset, other):
    count = lax.axis_size("x")
    at_x = lax.rem(lax.axis_index("x") + offset * turn() + count, count)
    return 2 * at_x + lax.rem(lax.axis_index("h") + other, 2)


def low(value):
    return value.astype(jnp.bfloat16)


def wide(value):
    return value.astype(jnp.float32)


def across(column):
    return jnp.broadcast_to(column, (column.shape[0], 128)).T[0:1, :]


def down(row):
    return jnp.broadcast_to(row, (128, row.shape[1])).T


def product(left, right, left_dim, right_dim):
    return lax.dot_general(
        left, right, (((left_dim,), (right_dim,)), ((), ())), preferred_element_type=jnp.float32
    )


def stage_kernel(scale_ref, cot_in, img_in, txt_in, *refs):
    cot_ref, img_ref, txt_ref, gi_ref, gt_ref, match_ref, sems = refs
    copies = [
        pltpu.make_async_copy(source, target, sems.at[k])
        for k, (source, target) in enumerate(
            ((img_in, img_ref), (txt_in, txt_ref), (cot_in, cot_ref))
        )
    ]
    for copy in copies:
        copy.start()
    for copy in copies:
        copy.wait()
    img, txt = wide(img_ref[...]), wide(txt_ref[...])
    both = down(cot_ref[0:1, :] + cot_ref[1:2, :])[:, 0:1]
    gi_ref[...] = both * txt
    gt_ref[...] = both * img
    match_ref[...] = across(scale_ref[0] * jnp.sum(img * txt, axis=1, keepdims=True))


def scores_into(scale_ref, img_ref, txt_ref, s_ref):
    for c in range(0, txt_ref.shape[0], 256):
        part = product(img_ref[...], txt_ref[c : c + 256, :], 1, 1)
        s_ref[:, c : c + 256] = scale_ref[0] * part
    return jnp.max(s_ref[...], axis=0, keepdims=True)


def stats_into(s_ref, row_ref, col_top):
    col_sum = jnp.zeros_like(col_top)
    for b in range(row_ref.shape[0]):
        s = s_ref[128 * b : 128 * b + 128, :]
        top = jnp.max(s, axis=1, keepdims=True)
        total = jnp.sum(jnp.exp(s - top), axis=1, keepdims=True)
        row_ref[b : b + 1, :] = across(top + jnp.log(total))
        col_sum = col_sum + jnp.sum(jnp.exp(s - col_top), axis=0, keepdims=True)
    return col_sum


def pack(refs, into):
    for b, ref in enumerate(refs):
        into[128 * b : 128 * b + 128, :] = ref[...]


def stats_a_kernel(blocks, scale_ref, *refs):
    s_ref, row_ref, top_ref, sum_ref, img_ref, txt_ref = refs[-6:]
    pack(refs[:blocks], img_ref)
    pack(refs[blocks:-6], txt_ref)
    col_top = scores_into(scale_ref, img_ref.at[: 128 * blocks, :], txt_ref, s_ref)
    top_ref[...] = col_top
    sum_ref[...] = stats_into(s_ref, row_ref, col_top)


def stats_b_kernel(offs, turns, late, scale_ref, cot_ref, *refs):
    row_a, txt_ref, top_ref, sum_ref, _, s_ref, row_ref, col_ref, img_all, row_b = refs[late:]
    img_ref = img_all.at[128 * (len(offs) - late) :, :]
    pack(refs[:late], img_ref)
    col_top = jnp.maximum(scores_into(scale_ref, img_ref, txt_ref, s_ref), top_ref[...])
    col_sum = stats_into(s_ref, row_b, col_top) + sum_ref[...] * jnp.exp(top_ref[...] - col_top)
    lse = col_top + jnp.log(col_sum)
    row_ref[...] = jnp.zeros_like(row_ref)
    col_ref[...] = jnp.zeros_like(col_ref)
    early = len(offs) - late
    for b, offset in enumerate(offs):
        part = row_a[b : b + 1, :] if b < early else row_b[b - early : b - early + 1, :]
        row_ref[pl.ds(image_id(offset), 1), :] = part
    for c, place in enumerate(turns):
        col_ref[pl.ds(text_id(*place), 1), :] = lse[:, 128 * c : 128 * c + 128]
    row_ref[pl.ds(len(offs) + image_id(0), 1), :] = cot_ref[0:1, :]
    col_ref[pl.ds(len(turns) + text_id(0, 0), 1), :] = cot_ref[1:2, :]


def weights_into(s_ref, w_ref, row_ref, col_ref, offs, turns):
    rows, cols = row_ref.shape[0] // 2, col_ref.shape[0] // 2
    places = [text_id(*place) for place in turns]
    col_lse = [col_ref[pl.ds(at, 1), :] for at in places]
    col_cot = [col_ref[pl.ds(cols + at, 1), :] for at in places]
    for b, offset in enumerate(offs):
        row_lse = down(row_ref[pl.ds(image_id(offset), 1), :])
        row_cot = down(row_ref[pl.ds(rows + image_id(offset), 1), :])
        for c in range(cols):
            s = s_ref[128 * b : 128 * b + 128, 128 * c : 128 * c + 128]
            w = row_cot * jnp.exp(s - row_lse) + col_cot[c] * jnp.exp(s - col_lse[c])
            w_ref[128 * b : 128 * b + 128, 128 * c : 128 * c + 128] = low(w)


def weights_kernel(
    offs, turns, sa_ref, sb_ref, row_ref, col_ref, img_ref, txt_ref, w_ref, *out_refs
):
    rows, width = sa_ref.shape
    split = rows // 128
    late = len(offs) - split
    weights_into(sb_ref, w_ref.at[rows:, :], row_ref, col_ref, offs[split:], turns)
    image_part = product(w_ref[rows:, :], txt_ref[...], 1, 0)
    for k in range(late):
        out_refs[k][...] = low(image_part[128 * k : 128 * k + 128, :])
    weights_into(sa_ref, w_ref.at[:rows, :], row_ref, col_ref, offs[:split], turns)
    text_part = product(w_ref[:, width - 256 :], img_ref[...], 0, 0)
    for k in range(2):
        out_refs[late + k][...] = low(text_part[128 * k : 128 * k + 128, :])


def rest_kernel(rows, cols, w_ref, img_ref, txt_ref, gi_ref, gt_ref, *refs):
    match_ref, row_ref, col_ref = refs[:3]
    out_refs, loss_ref = refs[3:-1], refs[-1]
    image_part = product(w_ref[: 128 * rows, :], txt_ref[...], 1, 0)
    out_refs[0][...] = image_part[:128, :] - gi_ref[...]
    for k in range(1, rows):
        out_refs[k][...] = image_part[128 * k : 128 * k + 128, :]
    text_part = product(w_ref[:, : 128 * cols], img_ref[...], 0, 0)
    out_refs[rows][...] = text_part[:128, :] - gt_ref[...]
    for k in range(1, cols):
        ref = out_refs[rows + k]
        ref[...] = text_part[128 * k : 128 * k + 128, :].astype(ref.dtype)
    loss_ref[0:1, :] = row_ref[pl.ds(image_id(0), 1), :] - match_ref[...]
    loss_ref[1:2, :] = col_ref[pl.ds(text_id(0, 0), 1), :] - match_ref[...]


def shape(*dims, dtype=jnp.float32):
    return jax.ShapeDtypeStruct(dims, dtype)


def call(kernel, specs, outs, flops, scratch=(), aliases=None):
    return pl.pallas_call(
        kernel,
        in_specs=specs,
        out_specs=[VMEM] * len(outs),
        out_shape=outs,
        scratch_shapes=scratch,
        input_output_aliases=aliases or {},
        compiler_params=PARAMS,
        cost_estimate=pl.CostEstimate(flops=flops, bytes_accessed=4 << 20, transcendentals=1 << 20),
    )


def merge_lse(first, second):
    top = jnp.maximum(first, second)
    return top + jnp.log(jnp.exp(first - top) + jnp.exp(second - top))


def step(images, texts, scale, cotangent):
    n, width = images.shape
    logit_scale = scale[0]
    z_n, x_n = lax.axis_size("z"), lax.axis_size("x")
    c_n = 2 * x_n
    half = z_n // 2
    offs = [0] + [s * k for k in range(1, half) for s in (1, -1)] + [half]
    turns = [(d, e) for d in (0, 1, -1, 2) for e in (0, 1)]
    rows, cols = z_n * n, c_n * n
    early = half + 1
    late = z_n - early
    tile = 2 * cols * width * n
    sent = shape(n, width, dtype=jnp.bfloat16)
    kept = shape(n, width)
    img_held = gather_z(images)
    txt_held = gather_xh(texts)
    cot, img_own, txt_own, base_i, base_t, matched = call(
        stage_kernel,
        [SMEM] + [pl.BlockSpec(memory_space=pltpu.HBM)] * 3,
        [shape(2, n), sent, sent, kept, kept, shape(1, n)],
        tile // 8,
        [pltpu.SemaphoreType.DMA((3,))],
    )(scale, *[pltpu.with_memory_space_constraint(v, pltpu.HBM) for v in (cotangent, images, texts)])
    img_held[0], txt_held[0, 0] = img_own, txt_own
    s_a, row_a, top_a, sum_a, img_a, txt = call(
        functools.partial(stats_a_kernel, early),
        [SMEM] + [VMEM] * (early + c_n),
        [shape(early * n, cols), shape(early, n), shape(1, cols), shape(1, cols)]
        + [shape(r, width, dtype=jnp.bfloat16) for r in (rows, cols)],
        early * tile,
    )(scale, *[img_held[o] for o in offs[:early]], *[txt_held[t] for t in turns])
    s_b, row_msg, col_msg, img = call(
        functools.partial(stats_b_kernel, offs, turns, late),
        [SMEM] + [VMEM] * (late + 6),
        [shape(late * n, cols), shape(2 * z_n, n), shape(2 * c_n, n)]
        + [shape(rows, width, dtype=jnp.bfloat16)],
        late * tile,
        [pltpu.VMEM((late, n), jnp.float32)],
        {late + 6: 3},
    )(scale, cot, *[img_held[o] for o in offs[early:]], row_a, txt, top_a, sum_a, img_a)

    def merged(mine, got, sums):
        return jnp.where(sums, mine + got, merge_lse(mine, got))

    row_sums = lax.broadcasted_iota(jnp.int32, row_msg.shape, 0) >= z_n
    col_sums = lax.broadcasted_iota(jnp.float32, col_msg.shape, 0) > c_n - 0.5
    for z_bit, col_axis, col_bit in ((7, "h", 1), (2, "x", 3), (1, "x", 1)):
        row_got = swapped(row_msg, "z", z_bit)
        col_got = swapped(col_msg, col_axis, col_bit)
        row_msg = merged(row_msg, row_got, row_sums)
        col_msg = merged(col_msg, col_got, col_sums)

    weights, up, down_msg, far, fore, back = call(
        functools.partial(weights_kernel, offs, turns),
        [VMEM] * 6,
        [shape(rows, cols, dtype=jnp.bfloat16)] + [sent] * (late + 2),
        4 * tile,
    )(s_a, s_b, row_msg, col_msg, img, txt)
    direct = ((1, 1), (-1, 0))
    parts = call(
        functools.partial(rest_kernel, early, c_n - 2),
        [VMEM] * 8,
        [kept] * early
        + [sent if t in direct else kept for t in turns[:-2]]
        + [shape(2, n)],
        12 * tile,
    )(weights, img, txt, base_i, base_t, matched, row_msg, col_msg)
    part = dict(zip(offs[:early], parts[:early]))
    piece = dict(zip(turns[:-2], parts[early:-1]))

    far = wide(moved(far, "z", half - 1))
    up = moved(up, "z", 1)
    down_msg = moved(down_msg, "z", -1)
    for k in range(half - 2, 0, -1):
        total = part[k] + wide(up)
        if k == 1:
            total = total + far
        up = moved(low(total), "z", 1)
        down_msg = moved(low(part[-k] + wide(down_msg)), "z", -1)
    img_terms = part[0] + wide(up) + wide(down_msg)

    fore = moved(fore, "x", 1)
    back = moved(back, "x", -1)
    fore1 = moved(piece[1, 1], "x", 1)
    back0 = moved(piece[-1, 0], "x", -1)
    fore0 = moved(low(piece[1, 0] + wide(fore)), "x", 1)
    back1 = moved(low(piece[-1, 1] + wide(back)), "x", -1)
    other = moved(low(piece[0, 1] + wide(fore1) + wide(back1)), "h", 1)

    grad_texts = logit_scale * (piece[0, 0] + wide(fore0) + wide(back0) + wide(other))
    return (parts[-1], logit_scale * img_terms, grad_texts)


def solution(mesh):
    grid = Mesh(mesh.devices.reshape(4, 8, 2, 4), ("x", "z", "h", "dp"))
    rows = ("dp", "x", "z", "h")
    return jax.shard_map(
        step,
        mesh=grid,
        in_specs=(P(rows, None), P(rows, None), P(), P(None, rows)),
        out_specs=(P(None, rows), P(rows, None), P(rows, None)),
        check_vma=False,
    )
```

```python
import functools

import jax
import jax.numpy as jnp
from jax import lax
from jax.experimental import pallas as pl
from jax.experimental.pallas import tpu as pltpu
from jax.sharding import Mesh, PartitionSpec as P

VMEM = pl.BlockSpec(memory_space=pltpu.VMEM)
SMEM = pl.BlockSpec(memory_space=pltpu.SMEM)
PARAMS = pltpu.CompilerParams(vmem_limit_bytes=24 * 1024 * 1024)


def moved(value, axis, steps):
    count, lanes = lax.axis_size(axis), lax.axis_size("dp")
    pairs = [
        (i * lanes + c, (i + (steps if c % 2 == 0 else -steps)) % count * lanes + c)
        for i in range(count)
        for c in range(lanes)
    ]
    return lax.ppermute(value, (axis, "dp"), pairs)


def swapped(value, axis, bit):
    count = lax.axis_size(axis)
    return lax.ppermute(value, axis, [(i, i ^ bit) for i in range(count)])


def gather_z(block):
    half = lax.axis_size("z") // 2
    held = {0: block}
    for k in range(1, half):
        held[-k] = moved(held[1 - k], "z", 1)
        held[k] = moved(held[k - 1], "z", -1)
    held[half] = moved(held[half - 2], "z", -2)
    return held


def gather_xh(block):
    held = {(0, 0): block, (0, 1): moved(block, "h", 1)}
    for e in (0, 1):
        held[1, e] = moved(held[0, e], "x", -1)
        held[-1, e] = moved(held[0, e], "x", 1)
    held[2, 0] = moved(held[1, 0], "x", -1)
    held[2, 1] = moved(held[-1, 1], "x", 1)
    return held


def turn():
    return 1 - 2 * lax.rem(lax.axis_index("dp"), 2)


def image_id(offset):
    count = lax.axis_size("z")
    return lax.rem(lax.axis_index("z") + offset * turn() + count, count)


def text_id(offset, other):
    count = lax.axis_size("x")
    at_x = lax.rem(lax.axis_index("x") + offset * turn() + count, count)
    return 2 * at_x + lax.rem(lax.axis_index("h") + other, 2)


def low(value):
    return value.astype(jnp.bfloat16)


def wide(value):
    return value.astype(jnp.float32)


def across(column):
    return jnp.broadcast_to(column, (column.shape[0], 128)).T[0:1, :]


def down(row):
    return jnp.broadcast_to(row, (128, row.shape[1])).T


def product(left, right, left_dim, right_dim):
    return lax.dot_general(
        left, right, (((left_dim,), (right_dim,)), ((), ())), preferred_element_type=jnp.float32
    )


def stage_kernel(scale_ref, cot_in, img_in, txt_in, *refs):
    cot_ref, img_ref, txt_ref, gi_ref, gt_ref, match_ref, sems = refs
    copies = [
        pltpu.make_async_copy(source, target, sems.at[k])
        for k, (source, target) in enumerate(
            ((img_in, img_ref), (txt_in, txt_ref), (cot_in, cot_ref))
        )
    ]
    for copy in copies:
        copy.start()
    for copy in copies:
        copy.wait()
    img, txt = wide(img_ref[...]), wide(txt_ref[...])
    both = down(cot_ref[0:1, :] + cot_ref[1:2, :])[:, 0:1]
    gi_ref[...] = both * txt
    gt_ref[...] = both * img
    match_ref[...] = across(scale_ref[0] * jnp.sum(img * txt, axis=1, keepdims=True))


def scores_into(scale_ref, img_ref, txt_ref, s_ref):
    for c in range(0, txt_ref.shape[0], 256):
        part = product(img_ref[...], txt_ref[c : c + 256, :], 1, 1)
        s_ref[:, c : c + 256] = scale_ref[0] * part
    return jnp.max(s_ref[...], axis=0, keepdims=True)


def stats_into(s_ref, row_ref, col_top):
    col_sum = jnp.zeros_like(col_top)
    for b in range(row_ref.shape[0]):
        s = s_ref[128 * b : 128 * b + 128, :]
        top = jnp.max(s, axis=1, keepdims=True)
        total = jnp.sum(jnp.exp(s - top), axis=1, keepdims=True)
        row_ref[b : b + 1, :] = across(top + jnp.log(total))
        col_sum = col_sum + jnp.sum(jnp.exp(s - col_top), axis=0, keepdims=True)
    return col_sum


def pack(refs, into):
    for b, ref in enumerate(refs):
        into[128 * b : 128 * b + 128, :] = ref[...]


def stats_a_kernel(blocks, scale_ref, *refs):
    s_ref, row_ref, top_ref, sum_ref, img_ref, txt_ref = refs[-6:]
    pack(refs[:blocks], img_ref)
    pack(refs[blocks:-6], txt_ref)
    col_top = scores_into(scale_ref, img_ref.at[: 128 * blocks, :], txt_ref, s_ref)
    top_ref[...] = col_top
    sum_ref[...] = stats_into(s_ref, row_ref, col_top)


def stats_b_kernel(offs, turns, late, scale_ref, cot_ref, *refs):
    row_a, txt_ref, top_ref, sum_ref, _, s_ref, row_ref, col_ref, img_all, row_b = refs[late:]
    img_ref = img_all.at[128 * (len(offs) - late) :, :]
    pack(refs[:late], img_ref)
    col_top = jnp.maximum(scores_into(scale_ref, img_ref, txt_ref, s_ref), top_ref[...])
    col_sum = stats_into(s_ref, row_b, col_top) + sum_ref[...] * jnp.exp(top_ref[...] - col_top)
    lse = col_top + jnp.log(col_sum)
    row_ref[...] = jnp.zeros_like(row_ref)
    col_ref[...] = jnp.zeros_like(col_ref)
    early = len(offs) - late
    for b, offset in enumerate(offs):
        part = row_a[b : b + 1, :] if b < early else row_b[b - early : b - early + 1, :]
        row_ref[pl.ds(image_id(offset), 1), :] = part
    for c, place in enumerate(turns):
        col_ref[pl.ds(text_id(*place), 1), :] = lse[:, 128 * c : 128 * c + 128]
    row_ref[pl.ds(len(offs) + image_id(0), 1), :] = cot_ref[0:1, :]
    col_ref[pl.ds(len(turns) + text_id(0, 0), 1), :] = cot_ref[1:2, :]


def weights_into(s_ref, w_ref, row_ref, col_ref, offs, turns):
    rows, cols = row_ref.shape[0] // 2, col_ref.shape[0] // 2
    places = [text_id(*place) for place in turns]
    col_lse = [col_ref[pl.ds(at, 1), :] for at in places]
    col_cot = [col_ref[pl.ds(cols + at, 1), :] for at in places]
    for b, offset in enumerate(offs):
        row_lse = down(row_ref[pl.ds(image_id(offset), 1), :])
        row_cot = down(row_ref[pl.ds(rows + image_id(offset), 1), :])
        for c in range(cols):
            s = s_ref[128 * b : 128 * b + 128, 128 * c : 128 * c + 128]
            w = row_cot * jnp.exp(s - row_lse) + col_cot[c] * jnp.exp(s - col_lse[c])
            w_ref[128 * b : 128 * b + 128, 128 * c : 128 * c + 128] = low(w)


def weights_kernel(
    offs, turns, sa_ref, sb_ref, row_ref, col_ref, img_ref, txt_ref, w_ref, *out_refs
):
    rows, width = sa_ref.shape
    split = rows // 128
    late = len(offs) - split
    weights_into(sb_ref, w_ref.at[rows:, :], row_ref, col_ref, offs[split:], turns)
    image_part = product(w_ref[rows:, :], txt_ref[...], 1, 0)
    for k in range(late):
        out_refs[k][...] = low(image_part[128 * k : 128 * k + 128, :])
    weights_into(sa_ref, w_ref.at[:rows, :], row_ref, col_ref, offs[:split], turns)
    text_part = product(w_ref[:, width - 256 :], img_ref[...], 0, 0)
    for k in range(2):
        out_refs[late + k][...] = low(text_part[128 * k : 128 * k + 128, :])


def rest_kernel(rows, cols, w_ref, img_ref, txt_ref, gi_ref, gt_ref, *refs):
    match_ref, row_ref, col_ref = refs[:3]
    out_refs, loss_ref = refs[3:-1], refs[-1]
    image_part = product(w_ref[: 128 * rows, :], txt_ref[...], 1, 0)
    out_refs[0][...] = image_part[:128, :] - gi_ref[...]
    for k in range(1, rows):
        out_refs[k][...] = image_part[128 * k : 128 * k + 128, :]
    text_part = product(w_ref[:, : 128 * cols], img_ref[...], 0, 0)
    out_refs[rows][...] = text_part[:128, :] - gt_ref[...]
    for k in range(1, cols):
        ref = out_refs[rows + k]
        ref[...] = text_part[128 * k : 128 * k + 128, :].astype(ref.dtype)
    loss_ref[0:1, :] = row_ref[pl.ds(image_id(0), 1), :] - match_ref[...]
    loss_ref[1:2, :] = col_ref[pl.ds(text_id(0, 0), 1), :] - match_ref[...]


def shape(*dims, dtype=jnp.float32):
    return jax.ShapeDtypeStruct(dims, dtype)


def call(kernel, specs, outs, flops, scratch=(), aliases=None):
    return pl.pallas_call(
        kernel,
        in_specs=specs,
        out_specs=[VMEM] * len(outs),
        out_shape=outs,
        scratch_shapes=scratch,
        input_output_aliases=aliases or {},
        compiler_params=PARAMS,
        cost_estimate=pl.CostEstimate(flops=flops, bytes_accessed=4 << 20, transcendentals=1 << 20),
    )


def merge_lse(first, second):
    top = jnp.maximum(first, second)
    return top + jnp.log(jnp.exp(first - top) + jnp.exp(second - top))


def step(images, texts, scale, cotangent):
    n, width = images.shape
    logit_scale = scale[0]
    z_n, x_n = lax.axis_size("z"), lax.axis_size("x")
    c_n = 2 * x_n
    half = z_n // 2
    offs = [0] + [s * k for k in range(1, half) for s in (1, -1)] + [half]
    turns = [(d, e) for d in (0, 1, -1, 2) for e in (0, 1)]
    rows, cols = z_n * n, c_n * n
    early = half + 1
    late = z_n - early
    tile = 2 * cols * width * n
    sent = shape(n, width, dtype=jnp.bfloat16)
    kept = shape(n, width)
    img_held = gather_z(images)
    txt_held = gather_xh(texts)
    cot, img_own, txt_own, base_i, base_t, matched = call(
        stage_kernel,
        [SMEM] + [pl.BlockSpec(memory_space=pltpu.HBM)] * 3,
        [shape(2, n), sent, sent, kept, kept, shape(1, n)],
        tile // 8,
        [pltpu.SemaphoreType.DMA((3,))],
    )(scale, *[pltpu.with_memory_space_constraint(v, pltpu.HBM) for v in (cotangent, images, texts)])
    img_held[0], txt_held[0, 0] = img_own, txt_own
    s_a, row_a, top_a, sum_a, img_a, txt = call(
        functools.partial(stats_a_kernel, early),
        [SMEM] + [VMEM] * (early + c_n),
        [shape(early * n, cols), shape(early, n), shape(1, cols), shape(1, cols)]
        + [shape(r, width, dtype=jnp.bfloat16) for r in (rows, cols)],
        early * tile,
    )(scale, *[img_held[o] for o in offs[:early]], *[txt_held[t] for t in turns])
    s_b, row_msg, col_msg, img = call(
        functools.partial(stats_b_kernel, offs, turns, late),
        [SMEM] + [VMEM] * (late + 6),
        [shape(late * n, cols), shape(2 * z_n, n), shape(2 * c_n, n)]
        + [shape(rows, width, dtype=jnp.bfloat16)],
        late * tile,
        [pltpu.VMEM((late, n), jnp.float32)],
        {late + 6: 3},
    )(scale, cot, *[img_held[o] for o in offs[early:]], row_a, txt, top_a, sum_a, img_a)

    def merged(mine, got, sums):
        return jnp.where(sums, mine + got, merge_lse(mine, got))

    row_sums = lax.broadcasted_iota(jnp.int32, row_msg.shape, 0) >= z_n
    col_sums = lax.broadcasted_iota(jnp.float32, col_msg.shape, 0) > c_n - 0.5
    for z_bit, col_axis, col_bit in ((7, "h", 1), (2, "x", 3), (1, "x", 1)):
        row_got = swapped(row_msg, "z", z_bit)
        col_got = swapped(col_msg, col_axis, col_bit)
        row_msg = merged(row_msg, row_got, row_sums)
        col_msg = merged(col_msg, col_got, col_sums)

    weights, up, down_msg, far, fore, back = call(
        functools.partial(weights_kernel, offs, turns),
        [VMEM] * 6,
        [shape(rows, cols, dtype=jnp.bfloat16)] + [sent] * (late + 2),
        4 * tile,
    )(s_a, s_b, row_msg, col_msg, img, txt)
    direct = ((1, 1), (-1, 0))
    parts = call(
        functools.partial(rest_kernel, early, c_n - 2),
        [VMEM] * 8,
        [kept] * early
        + [sent if t in direct else kept for t in turns[:-2]]
        + [shape(2, n)],
        12 * tile,
    )(weights, img, txt, base_i, base_t, matched, row_msg, col_msg)
    part = dict(zip(offs[:early], parts[:early]))
    piece = dict(zip(turns[:-2], parts[early:-1]))

    far = wide(moved(far, "z", 2))
    up = moved(up, "z", 1)
    down_msg = moved(down_msg, "z", -1)
    for k in range(half - 2, 0, -1):
        total = part[k] + wide(up)
        if k == half - 2:
            total = total + far
        up = moved(low(total), "z", 1)
        down_msg = moved(low(part[-k] + wide(down_msg)), "z", -1)
    img_terms = part[0] + wide(up) + wide(down_msg)

    fore = moved(fore, "x", 1)
    back = moved(back, "x", -1)
    fore1 = moved(piece[1, 1], "x", 1)
    back0 = moved(piece[-1, 0], "x", -1)
    fore0 = moved(low(piece[1, 0] + wide(fore)), "x", 1)
    back1 = moved(low(piece[-1, 1] + wide(back)), "x", -1)
    other = moved(low(piece[0, 1] + wide(fore1) + wide(back1)), "h", 1)

    grad_texts = logit_scale * (piece[0, 0] + wide(fore0) + wide(back0) + wide(other))
    return (parts[-1], logit_scale * img_terms, grad_texts)


def solution(mesh):
    grid = Mesh(mesh.devices.reshape(4, 8, 2, 4), ("x", "z", "h", "dp"))
    rows = ("dp", "x", "z", "h")
    return jax.shard_map(
        step,
        mesh=grid,
        in_specs=(P(rows, None), P(rows, None), P(), P(None, rows)),
        out_specs=(P(None, rows), P(rows, None), P(rows, None)),
        check_vma=False,
    )
```
